32 devices in a mesh: pool: 2 (over y), blk: 4 (over x, core), batch: 4 (over z).
Axes of the slice: x: 2, y: 2, z: 4, core: 2. Of those that a mesh axis runs over, the one named last changes fastest.
Arguments:
- prompt: bfloat16 [8, 512, 4096], P(('pool', 'batch'), 'blk'), may hold values from -40 to 40
- prompt_len: int32 [2, 4], P('pool', 'batch'), may hold values from 128 to 512
- dec_tokens: bfloat16 [4, 32, 4096], P(None, ('pool', 'batch')), may hold values from -40 to 40
- cache_k: bfloat16 [32, 4096, 1024], P(('pool', 'batch'), None, 'blk'), may hold values from -72 to 72
- cache_v: bfloat16 [32, 4096, 1024], P(('pool', 'batch'), None, 'blk'), may hold values from -6 to 6
- cache_len: int32 [32], P(('pool', 'batch')), may hold values from 1 to 4092
- assign: int32 [2, 4], P('pool', 'batch'), may hold values from 0 to 3, each once within a row
- slot: int32 [2, 4], P('pool', 'batch'), may hold values from 0 to 3
- gain: float32 [4096], replicated, may hold values from 0.5 to 1.5
- w_qkv: bfloat16 [4096, 6144], P(None, 'blk'), may hold values from -4 to 4
- w_out: bfloat16 [4096, 4096], P('blk'), may hold values from -0.09375 to 0.09375
Outputs:
- prefill_out: bfloat16 [8, 512, 4096], P(('pool', 'batch'), 'blk')
- dec_out: bfloat16 [4, 32, 4096], P(None, ('pool', 'batch'))
The draws below stay inside these ranges and needn't reach their ends.
Inputs may be any that keep to these rules, and one draw needn't show every extreme that they name: For each pool p, assign[p] is a permutation of the 4 stretch indices of the other pool.
All inputs are finite; a program needn't handle non-finite values.
Results may differ from the reference program's by a relative error of at most 0.011.
Values may be sent and summed in bfloat16 or wider, within the bound.
No kernel may reach another device: no remote copies, remote signals or barrier semaphores. Data moves between devices by JAX's collectives and lax.ppermute only.
A program may use at most 128 MiB of HBM per device.

```python
import jax
import jax.numpy as jnp
from jax import lax

D = 4096
HEADS = 32
KV_HEADS = 8
HEAD_DIM = 128
GROUP = 4
STRETCH = 512
R_DEV = 4
CACHE = 4096
STEPS = 4
GROUPS = 8
ROWS = 32
N_POOL = 2
N_BLK = 4
N_BATCH = 4


def draw_prompt(key, part):
    shape = (GROUPS, STRETCH, D)
    drawn = jax.random.truncated_normal(jax.random.fold_in(key, 4100), -6.0, 6.0, shape, jnp.float32)
    return drawn.astype(jnp.bfloat16)


def draw_dec_tokens(key, part):
    shape = (STEPS, ROWS, D)
    drawn = jax.random.truncated_normal(jax.random.fold_in(key, 4200), -6.0, 6.0, shape, jnp.float32)
    return drawn.astype(jnp.bfloat16)


def draw_cache_k(key, part):
    shape = (ROWS, CACHE, KV_HEADS, HEAD_DIM)
    drawn = jax.random.truncated_normal(jax.random.fold_in(key, 4300), -6.0, 6.0, shape, jnp.float32)
    return drawn.reshape(ROWS, CACHE, KV_HEADS * HEAD_DIM).astype(jnp.bfloat16)


def draw_w_qkv(key, part):
    width = KV_HEADS * (GROUP + 2) * HEAD_DIM
    drawn = jax.random.truncated_normal(jax.random.fold_in(key, 4400), -6.0, 6.0, (D, width), jnp.float32) * D ** (-0.5)
    return drawn.astype(jnp.bfloat16)


def place_ends(entries, own_key, least, high):
    place = [jax.random.randint(jax.random.fold_in(own_key, axis), (), 0, length) for axis, length in enumerate(entries.shape)]
    main_axis = entries.shape.index(max(entries.shape))
    next_to = place[:main_axis] + [(place[main_axis] + 1) % entries.shape[main_axis]] + place[main_axis + 1:]
    return entries.at[tuple(place)].set(least).at[tuple(next_to)].set(high)


def block_levels(rng, shape, cuts, low, high):
    level = 1.0
    for axis_at, blocks in cuts:
        draws = jax.random.uniform(jax.random.fold_in(jax.random.fold_in(rng, 6), axis_at), (blocks,), jnp.float32, low / len(cuts), high / len(cuts))
        level = level * jnp.repeat(jnp.exp(draws), shape[axis_at] // blocks).reshape((-1,) + (1,) * (len(shape) - 1 - axis_at))
    return level


def centred(own_key, shape, scale, bound, pieces=(), held_as=jnp.bfloat16):
    level = block_levels(own_key, shape, pieces, -0.22, 0.18) if pieces else 1.0
    result = jax.random.normal(own_key, shape, jnp.float32) * scale * level
    return jnp.minimum(jnp.maximum(result, -bound), bound).astype(held_as)


def setup_inputs(seed: int = 0) -> dict:
    arg_keys = jax.random.split(jax.random.key(seed), 12)
    prompt = draw_prompt(jax.random.fold_in(arg_keys[11], 71), 0)
    prompt_len = place_ends(jax.random.randint(arg_keys[1], (N_POOL, N_BATCH), STRETCH // 4, STRETCH + 1), jax.random.fold_in(arg_keys[1], 1), STRETCH // 4, STRETCH).astype(jnp.int32)
    dec_tokens = draw_dec_tokens(jax.random.fold_in(arg_keys[11], 71), 0)
    cache_k = draw_cache_k(jax.random.fold_in(arg_keys[11], 71), 0)
    cache_v = centred(arg_keys[4], (ROWS, CACHE, KV_HEADS * HEAD_DIM), 1.0, 6.0, ((0, 8), (2, 4)))
    cache_len = place_ends(jax.random.randint(arg_keys[5], (ROWS,), 1, CACHE - STEPS + 1), jax.random.fold_in(arg_keys[5], 1), 1, CACHE - STEPS).astype(jnp.int32)
    assign = jax.vmap(lambda own: jax.random.permutation(own, N_BATCH))(jax.random.split(arg_keys[6], N_POOL)).reshape((N_POOL, N_BATCH)).astype(jnp.int32)
    slot = place_ends(jax.random.randint(arg_keys[7], (N_POOL, N_BATCH), 0, R_DEV), jax.random.fold_in(arg_keys[7], 1), 0, R_DEV - 1).astype(jnp.int32)
    gain = jnp.clip(1.0 + 0.1 * jax.random.normal(arg_keys[8], (D,), jnp.float32), 0.5, 1.5)
    w_qkv = draw_w_qkv(jax.random.fold_in(arg_keys[11], 71), 0)
    w_out = centred(arg_keys[10], (HEADS * HEAD_DIM, D), (HEADS * HEAD_DIM) ** -0.5, 0.09375, ((0, 4),))
    return dict(prompt=prompt, prompt_len=prompt_len, dec_tokens=dec_tokens, cache_k=cache_k, cache_v=cache_v, cache_len=cache_len, assign=assign, slot=slot, gain=gain, w_qkv=w_qkv, w_out=w_out)


EPSILON = 1e-05
THETA = 500000.0

def rms_norm(values, gain):
    wide = values.astype(jnp.float32)
    factor = lax.rsqrt(lax.optimization_barrier(jnp.mean(wide * wide, axis=-1, keepdims=True)) + EPSILON)
    return (wide * factor * gain.astype(jnp.float32)).astype(jnp.bfloat16)

def rotate(vector, places):
    half = vector.shape[-1] // 2
    freqs = THETA ** (-jnp.arange(half, dtype=jnp.float32) / half)
    angles = places.astype(jnp.float32)[..., None] * freqs
    cosine = jnp.cos(angles)
    sine = jnp.sin(angles)
    first = vector[..., :half]
    second = vector[..., half:]
    return jnp.concatenate([first * cosine - second * sine, second * cosine + first * sine], axis=-1)

def softmax_weights(scores):
    top = lax.optimization_barrier(jnp.max(scores, axis=-1, keepdims=True))
    expo = jnp.exp(scores - top)
    return (expo / lax.optimization_barrier(jnp.sum(expo, axis=-1, keepdims=True))).astype(jnp.bfloat16)

def head_blocks(mixed, w_out):
    width = HEADS * HEAD_DIM // N_BLK
    total = jnp.zeros((mixed.shape[0], D), jnp.float32)
    for index in range(N_BLK):
        piece_term = jnp.dot(mixed[:, index * width:(index + 1) * width], w_out[index * width:(index + 1) * width], preferred_element_type=jnp.float32).astype(jnp.bfloat16)
        total = total + lax.optimization_barrier(piece_term).astype(jnp.float32)
    return total

def prefill_group(hidden, plen, gain, w_qkv, w_out):
    f32 = jnp.float32
    normed = rms_norm(hidden, gain)
    joined = jnp.dot(normed, w_qkv, preferred_element_type=f32)
    joined = joined.reshape(STRETCH, KV_HEADS, GROUP + 2, HEAD_DIM)
    places = jnp.arange(STRETCH, dtype=jnp.int32)
    query = rotate(joined[:, :, :GROUP], places[:, None, None]).astype(jnp.bfloat16)
    key = rotate(joined[:, :, GROUP], places[:, None]).astype(jnp.bfloat16)
    value = joined[:, :, GROUP + 1].astype(jnp.bfloat16)
    scale = HEAD_DIM ** (-0.5)
    scores = jnp.einsum('qhgd,khd->hgqk', query.astype(f32), key.astype(f32)) * scale
    allowed = (places[None, :] <= places[:, None]) & (places[None, :] < plen)
    scores = jnp.where(allowed, scores, -jnp.inf)
    probs = softmax_weights(scores)
    mixed = jnp.einsum('hgqk,khd->qhgd', probs.astype(f32), value.astype(f32)).astype(jnp.bfloat16)
    mixed = mixed.reshape(STRETCH, HEADS * HEAD_DIM)
    term = head_blocks(mixed, w_out)
    return ((hidden.astype(f32) + term).astype(jnp.bfloat16), key, value)

def decode_group(tokens, cache_key, cache_value, lengths, new_key, new_value, new_len, row_slot, gain, w_qkv, w_out):
    f32 = jnp.float32
    normed = rms_norm(tokens, gain)
    joined = jnp.dot(normed.reshape(STEPS * R_DEV, D), w_qkv, preferred_element_type=f32)
    joined = joined.reshape(STEPS, R_DEV, KV_HEADS, GROUP + 2, HEAD_DIM)
    fresh = jnp.arange(R_DEV, dtype=jnp.int32) == row_slot
    begin = jnp.where(fresh, new_len, lengths)
    places = begin[None, :] + jnp.arange(STEPS, dtype=jnp.int32)[:, None]
    query = rotate(joined[:, :, :, :GROUP], places[:, :, None, None]).astype(jnp.bfloat16)
    key = rotate(joined[:, :, :, GROUP], places[:, :, None]).astype(jnp.bfloat16)
    value = joined[:, :, :, GROUP + 1].astype(jnp.bfloat16)
    cache_key = cache_key.reshape(R_DEV, CACHE, KV_HEADS, HEAD_DIM).astype(f32)
    cache_value = cache_value.reshape(R_DEV, CACHE, KV_HEADS, HEAD_DIM).astype(f32)
    scale = HEAD_DIM ** (-0.5)
    wq = query.astype(f32)
    old = jnp.einsum('srhgd,rchd->srhgc', wq, cache_key) * scale
    span = jnp.arange(CACHE, dtype=jnp.int32)
    old_ok = (span[None, :] < lengths[:, None]) & jnp.logical_not(fresh)[:, None]
    old = jnp.where(old_ok[None, :, None, None, :], old, -jnp.inf)
    new = jnp.einsum('srhgd,chd->srhgc', wq, new_key.astype(f32)) * scale
    reach = jnp.arange(STRETCH, dtype=jnp.int32)
    new_ok = (reach[None, :] < new_len) & fresh[:, None]
    new = jnp.where(new_ok[None, :, None, None, :], new, -jnp.inf)
    own = jnp.einsum('srhgd,trhd->srhgt', wq, key.astype(f32)) * scale
    steps_ok = jnp.arange(STEPS)[None, :] <= jnp.arange(STEPS)[:, None]
    own = jnp.where(steps_ok[:, None, None, None, :], own, -jnp.inf)
    probs = softmax_weights(jnp.concatenate([old, new, own], axis=-1)).astype(f32)
    mixed = jnp.einsum('srhgc,rchd->srhgd', probs[..., :CACHE], cache_value)
    mixed = mixed + jnp.einsum('srhgc,chd->srhgd', probs[..., CACHE:CACHE + STRETCH], new_value.astype(f32))
    mixed = mixed + jnp.einsum('srhgt,trhd->srhgd', probs[..., CACHE + STRETCH:], value.astype(f32))
    mixed = mixed.astype(jnp.bfloat16).reshape(STEPS * R_DEV, HEADS * HEAD_DIM)
    term = jnp.dot(mixed, w_out, preferred_element_type=f32).reshape(STEPS, R_DEV, D)
    return (tokens.astype(f32) + term).astype(jnp.bfloat16)

def reference(prompt, prompt_len, dec_tokens, cache_k, cache_v, cache_len, assign, slot, gain, w_qkv, w_out):

    def one_prefill(item):
        return prefill_group(item[0], item[1], gain, w_qkv, w_out)
    prefill_out, new_keys, new_values = lax.map(one_prefill, (prompt, prompt_len.reshape(GROUPS)))
    groups = jnp.arange(GROUPS, dtype=jnp.int32)
    source = ((1 - groups // N_BATCH) * N_BATCH + assign.reshape(GROUPS)).astype(jnp.int32)
    taken_keys = jnp.take(new_keys, source, axis=0)
    taken_values = jnp.take(new_values, source, axis=0)
    taken_lens = jnp.take(prompt_len.reshape(GROUPS), source, axis=0)
    tokens = dec_tokens.reshape(STEPS, GROUPS, R_DEV, D).transpose(1, 0, 2, 3)
    cache_key = cache_k.reshape(GROUPS, R_DEV, CACHE, KV_HEADS * HEAD_DIM)
    cache_value = cache_v.reshape(GROUPS, R_DEV, CACHE, KV_HEADS * HEAD_DIM)
    lengths = cache_len.reshape(GROUPS, R_DEV)

    def one_decode(item):
        return decode_group(item[0], item[1], item[2], item[3], item[4], item[5], item[6], item[7], gain, w_qkv, w_out)
    decoded = lax.map(one_decode, (tokens, cache_key, cache_value, lengths, taken_keys, taken_values, taken_lens, slot.reshape(GROUPS)))
    dec_out = decoded.transpose(1, 0, 2, 3).reshape(STEPS, ROWS, D)
    return (prefill_out, dec_out)
```

```python
import functools

import jax
import jax.numpy as jnp
import numpy as np
from jax import lax
from jax.experimental import pallas as pl
from jax.experimental.pallas import tpu as pltpu
from jax.sharding import PartitionSpec as P


HEAD_DIM = 128
GROUP = 4
KINDS = GROUP + 2
PAIR = 2 * HEAD_DIM
BLOCKS = KINDS // 2
EPSILON = 1e-05
THETA = 500000.0
NEG = -1e30
SCALE = HEAD_DIM ** (-0.5)
OUT_COLS = 1024
f32 = jnp.float32
bf16 = jnp.bfloat16


VMEM = pl.BlockSpec(memory_space=pltpu.MemorySpace.VMEM)
SMEM = pl.BlockSpec(memory_space=pltpu.MemorySpace.SMEM)
HBM = pl.BlockSpec(memory_space=pltpu.MemorySpace.HBM)
ANY = pl.BlockSpec(memory_space=pl.ANY)


def dot(a, b):
    return jnp.dot(a, b, preferred_element_type=f32)


def dot_t(a, b):
    return lax.dot_general(a, b, (((1,), (1,)), ((), ())), preferred_element_type=f32)


def rot(u, cosine, sine):
    return u * cosine + pltpu.roll(u, HEAD_DIM // 2, 1) * sine


def angle_tables(places):
    half = HEAD_DIM // 2
    freqs = THETA ** (-jnp.arange(half, dtype=f32) / half)
    angles = places.astype(f32)[..., None] * freqs
    cosine, sine = jnp.cos(angles), jnp.sin(angles)
    return jnp.concatenate([cosine, cosine], -1), jnp.concatenate([-sine, sine], -1)


def fixed_tables(count):
    half = HEAD_DIM // 2
    freqs = np.float32(THETA) ** (-np.arange(half, dtype=np.float32) / np.float32(half))
    angles = np.arange(count, dtype=np.float32)[:, None] * freqs.astype(np.float32)
    cosine, sine = np.cos(angles).astype(np.float32), np.sin(angles).astype(np.float32)
    return np.concatenate([cosine, cosine], -1), np.concatenate([-sine, sine], -1)


def norm_rows(src, dst, offset, gain_ref):
    rows = src.shape[0]

    def step(i, _):
        at = pl.multiple_of(i * 16, 16)
        wide = src[pl.ds(at, 16), :].astype(f32)
        factor = lax.rsqrt(jnp.mean(wide * wide, axis=-1, keepdims=True) + EPSILON)
        to = pl.multiple_of(offset + i * 16, 16)
        dst[pl.ds(to, 16), :] = (wide * factor * gain_ref[...]).astype(bf16)
        return 0

    lax.fori_loop(0, rows // 16, step, 0, unroll=2)


def weight_copies(w_hbm, w_vmem, sems, width):
    return [
        pltpu.make_async_copy(
            w_hbm.at[:, pl.ds(j * width, width)], w_vmem.at[j], sems.at[j]
        )
        for j in range(w_vmem.shape[0])
    ]


def rotated_pair(acc, cosine, sine, j):
    cosine, sine = cosine[...], sine[...]
    first = rot(acc[:, :HEAD_DIM], cosine, sine)
    second = acc[:, HEAD_DIM:]
    if j % BLOCKS != BLOCKS - 1:
        second = rot(second, cosine, sine)
    return jnp.concatenate([first, second], axis=1).astype(bf16)


def load(pairs, sems):
    copies = [pltpu.make_async_copy(src, dst, sems.at[i]) for i, (src, dst) in enumerate(pairs)]
    for copy in copies:
        copy.start()
    return copies


def norm_token_rows(parts, gain_ref):
    out = []
    for part in parts:
        wide = part.astype(f32)
        factor = lax.rsqrt(jnp.mean(wide * wide, axis=-1, keepdims=True) + EPSILON)
        out.append(wide * factor * gain_ref[...])
    return jnp.concatenate(out, axis=0).astype(bf16)


def first_kernel(
    idx, own_hbm, sib_hbm, dec_hbm, gain_hbm, cos_hbm, sin_hbm, wq_hbm, wo_hbm,
    _a, _b, _c, _d, _e, own_out, sib_out, raw_out, wq, wo, later_hbm,
    own, sib, dec, gain, tabs, normed, q_sems, o_sems, in_sems, later_sem,
):
    rows = own.shape[0]
    steps, decs = dec.shape[:2]
    at = [pl.ds(pl.multiple_of(idx[i] * rows, rows), rows) for i in range(2)]
    weights = weight_copies(wq_hbm, wq, q_sems, PAIR) + weight_copies(wo_hbm, wo, o_sems, OUT_COLS)
    ready = load([(gain_hbm, gain), (own_hbm, own), (dec_hbm, dec), (sib_hbm, sib)], in_sems)
    for i in range(2):
        ready += load(
            [(cos_hbm.at[at[i]], tabs.at[2 * i]), (sin_hbm.at[at[i]], tabs.at[2 * i + 1])],
            in_sems.at[pl.ds(4 + 2 * i, 2)],
        )
    weights[0].start()
    ready[0].wait()
    ready[1].wait()
    through = pltpu.make_async_copy(own, later_hbm, later_sem)
    through.start()
    weights[1].start()
    norm_rows(own, normed, 0, gain)
    ready[2].wait()
    normed[2 * rows :] = norm_token_rows([dec[s] for s in range(steps)], gain)
    ready[3].wait()
    weights[2].start()
    norm_rows(sib, normed, rows, gain)
    for copy in ready[4:]:
        copy.wait()
    for j in range(wq.shape[0]):
        weights[j].wait()
        if j + 3 < len(weights):
            weights[j + 3].start()
        acc = dot(normed[...], wq[j])
        own_out[j] = rotated_pair(acc[:rows], tabs.at[0], tabs.at[1], j)
        sib_out[j] = rotated_pair(acc[rows : 2 * rows], tabs.at[2], tabs.at[3], j)
        for r in range(decs):
            for s in range(steps):
                row = 2 * rows + s * decs + r
                raw_out[r, j, s : s + 1] = acc[row : row + 1]
    for j in range(wq.shape[0], len(weights)):
        weights[j].wait()
        if j + 3 < len(weights):
            weights[j + 3].start()
    through.wait()


def own_tail(q, k_own, steps):
    s = dot_t(q, k_own) * SCALE
    at = lax.broadcasted_iota(jnp.int32, s.shape, 0)
    t = lax.broadcasted_iota(jnp.int32, s.shape, 1)
    return jnp.where(t <= lax.rem(at, steps), s, NEG)


def stacked_queries(raw, h, cosine, sine):
    parts = []
    for g in range(GROUP):
        block = raw(h * BLOCKS + g // 2)
        parts.append(rot(block[:, (g % 2) * HEAD_DIM : (g % 2 + 1) * HEAD_DIM], cosine, sine))
    return jnp.concatenate(parts, axis=0).astype(bf16)


def own_pair(raw, h, cosine, sine, pad):
    block = raw(h * BLOCKS + BLOCKS - 1)
    key = rot(block[:, :HEAD_DIM], cosine, sine)
    fill = jnp.zeros((pad - key.shape[0], HEAD_DIM), f32)
    key = jnp.concatenate([key, fill], axis=0).astype(bf16)
    value = jnp.concatenate([block[:, HEAD_DIM:], fill], axis=0).astype(bf16)
    return key, value


def decode_kernel(
    lens, slot, raw_ref, cos_ref, sin_ref, k_hbm, v_hbm,
    out_ref, k_s, v_s, q_s, ko_s, vo_s, m_s, l_s, acc_s, k_sem, v_sem,
):
    n_rows, count, width = k_s.shape[:3]
    steps = raw_ref.shape[2]
    heads = k_s.shape[3] // HEAD_DIM
    many = GROUP * steps

    def copies(r, j):
        at = pl.ds(j * width, width)
        return (
            pltpu.make_async_copy(k_hbm.at[r, at], k_s.at[r, j], k_sem.at[r, j]),
            pltpu.make_async_copy(v_hbm.at[r, at], v_s.at[r, j], v_sem.at[r, j]),
        )

    def live(r, j):
        return (j * width < lens[r]) & (slot[0, 0] != r)

    def fetch(r):
        for j in range(count):

            @pl.when(live(r, j))
            def _(r=r, j=j):
                for copy in copies(r, j):
                    copy.start()

    for r in range(min(2, n_rows)):
        fetch(r)
    for r in range(n_rows):
        raw = lambda b, r=r: raw_ref[r, b]
        q_s[r] = jnp.zeros_like(q_s[r])
        for h in range(heads):
            lanes = slice(h * HEAD_DIM, (h + 1) * HEAD_DIM)
            q_s[r, h * many : (h + 1) * many, lanes] = stacked_queries(raw, h, cos_ref[r], sin_ref[r])
            key, value = own_pair(raw, h, cos_ref[r], sin_ref[r], ko_s.shape[1])
            ko_s[r, :, lanes] = key
            vo_s[r, :, lanes] = value
    for r in range(n_rows):
        s = own_tail(q_s[r], ko_s[r], steps)
        m = jnp.max(s, axis=-1, keepdims=True)
        e = jnp.exp(s - m)
        m_s[r] = m
        l_s[r] = jnp.sum(e, axis=-1, keepdims=True)
        acc_s[r] = dot(e.astype(bf16), vo_s[r])

    for r in range(n_rows):
        for j in range(count):

            @pl.when(live(r, j))
            def _(r=r, j=j):
                k_copy, v_copy = copies(r, j)
                k_copy.wait()
                s = dot_t(q_s[r], k_s[r, j]) * SCALE
                at = j * width + lax.broadcasted_iota(jnp.int32, s.shape, 1)
                s = jnp.where(at < lens[r], s, NEG)
                m = jnp.maximum(m_s[r], jnp.max(s, axis=-1, keepdims=True))
                fade = jnp.exp(m_s[r] - m)
                e = jnp.exp(s - m)
                m_s[r] = m
                l_s[r] = l_s[r] * fade + jnp.sum(e, axis=-1, keepdims=True)
                v_copy.wait()
                acc_s[r] = acc_s[r] * fade + dot(e.astype(bf16), v_s[r, j])

        if r + 2 < n_rows:
            fetch(r + 2)

    for r in range(n_rows):
        mixed = acc_s[r] / l_s[r]
        for h in range(heads):
            for g in range(GROUP):
                to = (h * GROUP + g) * HEAD_DIM
                for s in range(steps):
                    at = h * many + g * steps + s
                    row = s * n_rows + r
                    out_ref[row : row + 1, to : to + HEAD_DIM] = mixed[
                        at : at + 1, h * HEAD_DIM : (h + 1) * HEAD_DIM
                    ]


def attend(queries, q_shard, pieces, plen, out_ref, offset, heads):
    for h in range(heads):
        parts = []
        for g in range(GROUP):
            block = queries(h * BLOCKS + g // 2)
            parts.append(block[:, (g % 2) * HEAD_DIM : (g % 2 + 1) * HEAD_DIM])
        rows = parts[0].shape[0]
        q = jnp.concatenate(parts, axis=0)
        q_at = q_shard * rows + lax.rem(lax.broadcasted_iota(jnp.int32, (GROUP * rows, 1), 0), rows)
        scores, values = [], []
        for kv, shard in pieces:
            pair = kv(h)
            count = pair.shape[0]
            k_at = shard * count + lax.broadcasted_iota(jnp.int32, (1, count), 1)
            k_at = jnp.where(k_at < plen, k_at, jnp.int32(1 << 30))
            s = dot_t(q, pair[:, :HEAD_DIM]) * SCALE
            scores.append(jnp.where(k_at <= q_at, s, NEG))
            values.append(pair[:, HEAD_DIM:])
        top = functools.reduce(jnp.maximum, scores)
        top = jnp.max(top, axis=-1, keepdims=True)
        total, mixed = None, None
        for s, value in zip(scores, values):
            e = jnp.exp(s - top)
            total = e if total is None else total + e
            term = dot(e.astype(bf16), value)
            mixed = term if mixed is None else mixed + term
        mixed = (mixed / jnp.sum(total, axis=-1, keepdims=True)).astype(bf16)
        for g in range(GROUP):
            to = (h * GROUP + g) * HEAD_DIM
            out_ref[offset : offset + rows, to : to + HEAD_DIM] = mixed[g * rows : (g + 1) * rows]


def attend_new(raw, cosine, sine, pieces, plen, out_ref, heads, steps):
    spread = out_ref.shape[0] // steps
    for h in range(heads):
        q = stacked_queries(raw, h, cosine, sine)
        key, value = own_pair(raw, h, cosine, sine, 16)
        scores, values = [own_tail(q, key, steps)], [value]
        for kv, shard in pieces:
            pair = kv(h)
            count = pair.shape[0]
            k_at = shard * count + lax.broadcasted_iota(jnp.int32, (1, count), 1)
            s = dot_t(q, pair[:, :HEAD_DIM]) * SCALE
            scores.append(jnp.where(k_at < plen, s, NEG))
            values.append(pair[:, HEAD_DIM:])
        top = functools.reduce(jnp.maximum, [jnp.max(s, axis=-1, keepdims=True) for s in scores])
        total, mixed = 0.0, 0.0
        for s, v in zip(scores, values):
            e = jnp.exp(s - top)
            total = total + jnp.sum(e, axis=-1, keepdims=True)
            mixed = mixed + dot(e.astype(bf16), v)
        mixed = mixed / total
        for g in range(GROUP):
            to = (h * GROUP + g) * HEAD_DIM
            rows = [
                jnp.broadcast_to(mixed[g * steps + s : g * steps + s + 1], (spread, HEAD_DIM))
                for s in range(steps)
            ]
            out_ref[:, to : to + HEAD_DIM] = jnp.concatenate(rows, axis=0).astype(bf16)


def chunk_kernel(which, n_full, n_kv, n_ask, answers, kv_only, *refs):
    refs = list(refs)
    take = lambda n: [refs.pop(0) for _ in range(n)]
    idx, plen, there, passed, gain_hbm, cos_hbm, sin_hbm, wq, wo = take(9)
    full, kvs, asks = take(n_full), take(n_kv), take(n_ask)
    new_raw, new_cos, new_sin = take(3) if answers else (None,) * 3
    take(1)
    kv_out = take(1)[0]
    part_out = None if kv_only else take(1)[0]
    raw_out = take(1)[0] if n_ask else None
    new_out = take(1)[0] if answers else None
    x, gain, tabs, normed, qkv, in_sem = take(6)
    attn = None if kv_only else take(1)[0]
    rows = x.shape[0]
    heads = kv_out.shape[0]
    shard = idx[which]
    at = pl.ds(pl.multiple_of(shard * rows, rows), rows)
    direct = lax.rem(idx[0], 2) == (which - n_full) % 2

    @pl.when(direct)
    def _():
        pltpu.make_async_copy(there, x, in_sem.at[0]).start()

    @pl.when(jnp.logical_not(direct))
    def _():
        pltpu.make_async_copy(passed, x, in_sem.at[0]).start()

    gain_copy = pltpu.make_async_copy(gain_hbm, gain, in_sem.at[1])
    gain_copy.start()
    tab_copies = [
        pltpu.make_async_copy(cos_hbm.at[at], tabs.at[0], in_sem.at[2]),
        pltpu.make_async_copy(sin_hbm.at[at], tabs.at[1], in_sem.at[3]),
    ]
    for copy in tab_copies:
        copy.start()
    gain_copy.wait()
    if n_ask:
        here = idx[idx.shape[0] - 1].astype(f32)
        steps = asks[0].shape[0] // 2
        new = jnp.zeros((steps, x.shape[1]), f32)
        for ref in asks:
            wide = ref[...].astype(f32)
            new = jnp.where(wide[steps : steps + 1] == here, wide[:steps], new)
        fill = jnp.zeros((16 - steps, x.shape[1]), f32)
        normed[rows:] = norm_token_rows([new, fill], gain)
    pltpu.make_async_copy(there, x, in_sem.at[0]).wait()
    norm_rows(x, normed, 0, gain)
    for copy in tab_copies:
        copy.wait()

    for j in range(wq.shape[0]):
        acc = dot(normed[...], wq[j])
        qkv[j] = rotated_pair(acc[:rows], tabs.at[0], tabs.at[1], j)
        if n_ask:
            raw_out[j] = acc[rows : rows + raw_out.shape[1]]
    for h in range(heads):
        kv_out[h] = qkv[h * BLOCKS + BLOCKS - 1]
    if kv_only:
        return
    pieces = [(lambda h, ref=ref: ref[h * BLOCKS + BLOCKS - 1], idx[i]) for i, ref in enumerate(full)]
    pieces += [(lambda h, ref=ref: ref[h], at) for ref, at in zip(kvs, kv_places(idx, which, n_full, n_kv))]
    pieces += [(lambda h: qkv[h * BLOCKS + BLOCKS - 1], shard)]
    if answers:
        steps = new_cos.shape[0]
        raw = lambda b: new_raw[b, :steps]
        attend_new(raw, new_cos[...], new_sin[...], pieces, plen[0, 0], new_out, heads, steps)
    attend(lambda b: qkv[b], shard, pieces, plen[0, 0], attn, 0, heads)

    for j in range(wo.shape[0]):
        part_out[:, j * OUT_COLS : (j + 1) * OUT_COLS] = dot(attn[...], wo[j]).astype(bf16)


def kv_places(idx, which, first, count):
    others = [i for i in range(first, first + count + 1) if i != which]
    return [idx[i] for i in others[:count]]


def last_kernel(n_kv, n_ret, n_rows, *refs):
    refs = list(refs)
    take = lambda n: [refs.pop(0) for _ in range(n)]
    idx, plen, slot, assign, own, sib = take(6)
    kvs = take(n_kv)
    dec, = take(1)
    rets = take(n_ret)
    wo, own_part, sib_part, dec_part, attn = take(5)
    rows = own.shape[1]
    heads = kvs[0].shape[0]
    pieces = [(lambda h, ref=ref: ref[h * BLOCKS + BLOCKS - 1], idx[i]) for i, ref in enumerate((own, sib))]
    pieces += [(lambda h, ref=ref: ref[h], idx[2 + i]) for i, ref in enumerate(kvs)]
    for i, ref in enumerate((own, sib)):
        attend(lambda b, ref=ref: ref[b], idx[i], pieces, plen[0, 0], attn, i * rows, heads)
    pick = lax.rem(idx[idx.shape[0] - 1] - assign[0, 0] + n_ret, n_ret)
    new = rets[0][...].astype(f32)
    for k in range(1, n_ret):
        new = jnp.where(pick == k, rets[k][...].astype(f32), new)
    at = lax.rem(lax.broadcasted_iota(jnp.int32, dec.shape, 0), n_rows)
    attn[2 * rows :] = jnp.where(at == slot[0, 0], new, dec[...]).astype(bf16)
    for j in range(wo.shape[0]):
        part = dot(attn[...], wo[j]).astype(bf16)
        cols = slice(j * OUT_COLS, (j + 1) * OUT_COLS)
        own_part[:, cols] = part[:rows]
        sib_part[:, cols] = part[rows:]
        dec_part[:, cols] = part[2 * rows :]


def add_kernel(start, a, b, out):
    rows = out.shape[0]

    def step(i, _):
        at = pl.ds(pl.multiple_of(i * 16, 16), 16)
        to = pl.ds(pl.multiple_of(start + i * 16, 16), 16)
        out[at, :] = (a[at, :].astype(f32) + b[to, :].astype(f32)).astype(bf16)
        return 0

    lax.fori_loop(0, rows // 16, step, 0)


def base_kernel(shard_hbm, own, sib, out, shard, sem):
    copy = pltpu.make_async_copy(shard_hbm, shard, sem)
    copy.start()
    copy.wait()

    def step(i, _):
        at = pl.ds(pl.multiple_of(i * 16, 16), 16)
        out[at, :] = shard[at, :].astype(f32) + own[at, :].astype(f32) + sib[at, :].astype(f32)
        return 0

    lax.fori_loop(0, out.shape[0] // 16, step, 0)


def sum_kernel(count, idx, base, *refs):
    parts, out, got, sems, out_sem = refs[: 2 * count], *refs[2 * count :]
    pieces = sems.shape[1]
    rows = out.shape[0] // pieces
    core = lax.rem(idx[0], 2)
    for k in range(2):

        @pl.when(core == k)
        def _(k=k):
            for n in range(pieces):
                at = pl.ds(n * rows, rows)
                for d in range(count):
                    pltpu.make_async_copy(parts[2 * d + k].at[at], got.at[d, at], sems.at[d, n]).start()

    done = []
    for n in range(pieces):
        at = slice(n * rows, (n + 1) * rows)
        total = base[at]
        for d in range(count):
            pltpu.make_async_copy(parts[2 * d].at[pl.ds(n * rows, rows)], got.at[d, at], sems.at[d, n]).wait()
            total = total + got[d, at].astype(f32)
        got[0, at] = total.astype(bf16)
        done.append(pltpu.make_async_copy(got.at[0, at], out.at[pl.ds(n * rows, rows)], out_sem.at[n]))
        done[-1].start()
    for copy in done:
        copy.wait()


def dec_kernel(tokens, a, b, out):
    steps, n_rows = tokens.shape[:2]
    total = a[...].astype(f32) + b[...].astype(f32)
    for s in range(steps):
        rows = total[s * n_rows : (s + 1) * n_rows]
        out[s] = (tokens[s].astype(f32) + rows).astype(bf16)


def params(mib):
    return pltpu.CompilerParams(vmem_limit_bytes=mib << 20)


def layer(
    prompt, prompt_len, dec_tokens, cache_k, cache_v, cache_len, assign, slot, gain, w_qkv, w_out
):
    n_blk, n_pool, n_batch = lax.axis_size("blk"), lax.axis_size("pool"), lax.axis_size("batch")
    n_chip = n_blk // 2
    shard = prompt[0]
    rows, width = shard.shape
    steps, n_rows = dec_tokens.shape[:2]
    heads = w_qkv.shape[1] // (KINDS * HEAD_DIM)
    blocks = heads * BLOCKS
    attn_cols = heads * GROUP * HEAD_DIM
    out_blocks = width // OUT_COLS
    decs = steps * n_rows

    blk = lax.axis_index("blk")
    chip, core = blk // 2, blk % 2
    batch = lax.axis_index("batch")
    at = jnp.arange(n_blk + 1, dtype=jnp.int32)
    far = (chip + n_chip - at // 2) % n_chip
    idx = jnp.where(at < 2, 2 * chip + (core + at) % 2, 2 * far + at % 2)
    idx = jnp.where(at == n_blk, batch, idx).astype(jnp.int32)
    gain_row = gain.reshape(1, width)
    cos_t, sin_t = (jnp.asarray(t) for t in fixed_tables(n_blk * rows))
    place = cache_len[:, None] + jnp.arange(steps, dtype=jnp.int32)[None, :]
    dec_cos, dec_sin = angle_tables(place)
    new_cos, new_sin = angle_tables(prompt_len[0, 0] + jnp.arange(steps, dtype=jnp.int32))

    swap = [(i, i ^ 1) for i in range(n_blk)]
    hop = lambda k, d: [(2 * c + k, 2 * ((c + d) % n_chip) + k) for c in range(n_chip)]
    toward = lambda k: [(2 * c + 1 - k, 2 * c + k) for c in range(n_chip)]
    shift = [
        [
            (p * n_batch + b, ((p + n_pool // 2) % n_pool) * n_batch + (b + k) % n_batch)
            for p in range(n_pool)
            for b in range(n_batch)
        ]
        for k in range(n_batch)
    ]
    groups = ("pool", "batch")
    near = lambda x: pltpu.with_memory_space_constraint(x, pltpu.MemorySpace.VMEM)
    stay = lambda x: pltpu.with_memory_space_constraint(x, pltpu.MemorySpace.HBM)

    row = lax.dynamic_index_in_dim(dec_tokens, slot[0, 0], 1, keepdims=False)
    wanted = jnp.full((steps, width), assign[0, 0]).astype(bf16)
    ask = jnp.concatenate([row, wanted], axis=0)
    sib_x = lax.ppermute(shard, "blk", swap)
    order = [(d, k) for d in range(1, n_chip) for k in range(2)]
    far_x = {}
    for d, k in order:
        if k == 0:
            far_x[d, k] = lax.ppermute(shard, "blk", hop(k, d))
    asks = [lax.ppermute(ask, groups, perm) for perm in shift]

    own, sib, raw, wq, wo, shard_later = pl.pallas_call(
        first_kernel,
        in_specs=[SMEM] + [HBM] * 8 + [ANY] * 5,
        out_specs=[VMEM] * 5 + [HBM],
        out_shape=[
            jax.ShapeDtypeStruct((blocks, rows, PAIR), bf16),
            jax.ShapeDtypeStruct((blocks, rows, PAIR), bf16),
            jax.ShapeDtypeStruct((n_rows, blocks, steps, PAIR), f32),
            pltpu.VMEM((blocks, width, PAIR), bf16),
            pltpu.VMEM((out_blocks, attn_cols, OUT_COLS), bf16),
            jax.ShapeDtypeStruct((rows, width), bf16),
        ],
        scratch_shapes=[
            pltpu.VMEM((rows, width), bf16),
            pltpu.VMEM((rows, width), bf16),
            pltpu.VMEM((steps, n_rows, width), bf16),
            pltpu.VMEM((1, width), f32),
            pltpu.VMEM((4, rows, HEAD_DIM), f32),
            pltpu.VMEM((2 * rows + decs, width), bf16),
            pltpu.SemaphoreType.DMA((blocks,)),
            pltpu.SemaphoreType.DMA((out_blocks,)),
            pltpu.SemaphoreType.DMA((8,)),
            pltpu.SemaphoreType.DMA,
        ],
        compiler_params=params(10),
        name="first",
    )(
        idx, stay(shard), sib_x, stay(dec_tokens), stay(gain_row), stay(cos_t), stay(sin_t),
        stay(w_qkv), stay(w_out), ask, dec_cos, dec_sin, new_cos, new_sin,
    )
    for d, k in order:
        if k == 1:
            far_x[d, k] = lax.ppermute(shard_later, "blk", hop(k, d))

    cached = cache_k.shape[1]
    step_rows = min(2048, cached)
    count = cached // step_rows
    kv_width = heads * HEAD_DIM
    many = GROUP * steps * heads
    dec_attn = pl.pallas_call(
        decode_kernel,
        in_specs=[SMEM] * 2 + [VMEM] * 3 + [HBM] * 2,
        out_specs=VMEM,
        out_shape=jax.ShapeDtypeStruct((decs, attn_cols), f32),
        scratch_shapes=[
            pltpu.VMEM((n_rows, count, step_rows, kv_width), bf16),
            pltpu.VMEM((n_rows, count, step_rows, kv_width), bf16),
            pltpu.VMEM((n_rows, many, kv_width), bf16),
            pltpu.VMEM((n_rows, 16, kv_width), bf16),
            pltpu.VMEM((n_rows, 16, kv_width), bf16),
            pltpu.VMEM((n_rows, many, 1), f32),
            pltpu.VMEM((n_rows, many, 1), f32),
            pltpu.VMEM((n_rows, many, kv_width), f32),
            pltpu.SemaphoreType.DMA((n_rows, count)),
            pltpu.SemaphoreType.DMA((n_rows, count)),
        ],
        compiler_params=params(20),
        name="decode",
    )(cache_len, slot, raw, dec_cos, dec_sin, stay(cache_k), stay(cache_v))

    def chunk(i, k, x, kvs, asks, answer, turn, kv_only):
        passed = lax.ppermute(x, "blk", [(b, a) for a, b in toward(k)])
        outs = [jax.ShapeDtypeStruct((heads, rows, PAIR), bf16)]
        tall = rows + (16 if asks else 0)
        scratch = [
            pltpu.VMEM((rows, width), bf16),
            pltpu.VMEM((1, width), f32),
            pltpu.VMEM((2, rows, HEAD_DIM), f32),
            pltpu.VMEM((tall, width), bf16),
            pltpu.VMEM((blocks, rows, PAIR), bf16),
            pltpu.SemaphoreType.DMA((4,)),
        ]
        if not kv_only:
            outs.append(jax.ShapeDtypeStruct((rows, width), bf16))
            scratch.append(pltpu.VMEM((rows, attn_cols), bf16))
        if asks:
            outs.append(jax.ShapeDtypeStruct((blocks, 8, PAIR), f32))
        if answer:
            outs.append(jax.ShapeDtypeStruct((decs, attn_cols), bf16))
        kernel = functools.partial(
            chunk_kernel, i, 2, len(kvs), len(asks), bool(answer), kv_only
        )
        extra = [*kvs, *asks, *answer]
        return pl.pallas_call(
            kernel,
            in_specs=[SMEM] * 2 + [HBM] * 5 + [VMEM] * (4 + len(extra)) + [ANY],
            out_specs=[VMEM] * len(outs),
            out_shape=outs,
            scratch_shapes=scratch,
            compiler_params=params(12),
            name="chunk",
        )(
            idx, prompt_len, x, passed, stay(gain_row), stay(cos_t), stay(sin_t),
            near(wq), near(wo), own, sib, *extra, turn,
        )

    def add(a, b, start=0):
        return pl.pallas_call(
            functools.partial(add_kernel, start),
            in_specs=[VMEM] * 2,
            out_specs=VMEM,
            out_shape=jax.ShapeDtypeStruct(a.shape, bf16),
            compiler_params=params(8),
            name="add",
        )(a, b)

    kvs, back = [], []
    ahead = n_chip > 2
    if ahead:
        kvs = [
            chunk(2 + i, k, far_x[d, k], [], [], [], gain_row, True)[0]
            for i, (d, k) in enumerate(order)
        ]
    turn, new_raw, fresh = gain_row, None, None
    for i, (d, k) in enumerate(order):
        final = i == len(order) - 1
        others = [kv for n, kv in enumerate(kvs) if n != i]
        outs = chunk(
            2 + i, k, far_x[d, k], others, asks if i == 0 else [],
            [new_raw, new_cos, new_sin] if final else [], turn, False,
        )
        if not ahead:
            kvs.append(outs[0])
        if i == 0:
            new_raw = outs[2]
        if final:
            fresh = outs[-1]
        other = lax.ppermute(outs[1], "blk", toward(k))
        turn = add(outs[1], other)
        back.append(lax.ppermute(turn, "blk", hop(k, n_chip - d)))

    rets = [lax.ppermute(fresh, groups, perm) for perm in shift]
    own_part, sib_part, dec_part = pl.pallas_call(
        functools.partial(last_kernel, len(kvs), n_batch, n_rows),
        in_specs=[SMEM] * 4 + [VMEM] * (4 + len(kvs) + n_batch),
        out_specs=[VMEM] * 3,
        out_shape=[
            jax.ShapeDtypeStruct((rows, width), bf16),
            jax.ShapeDtypeStruct((rows + decs, width), bf16),
            jax.ShapeDtypeStruct((decs, width), bf16),
        ],
        scratch_shapes=[
            pltpu.VMEM((2 * rows + decs, attn_cols), bf16),
        ],
        compiler_params=params(12),
        name="last",
    )(idx, prompt_len, slot, assign, own, sib, *kvs, dec_attn, *rets, near(wo))
    from_sib = lax.ppermute(sib_part, "blk", swap)

    total = add(dec_part, from_sib, rows)
    reach = 1
    while reach < n_chip:
        other = lax.ppermute(total, "blk", [(i, i ^ (2 * reach)) for i in range(n_blk)])
        reach *= 2
        if reach < n_chip:
            total = add(total, other)
    dec_out = pl.pallas_call(
        dec_kernel,
        in_specs=[VMEM] * 3,
        out_specs=VMEM,
        out_shape=jax.ShapeDtypeStruct(dec_tokens.shape, bf16),
        compiler_params=params(8),
        name="dec",
    )(dec_tokens, total, other)
    base = pl.pallas_call(
        base_kernel,
        in_specs=[HBM, VMEM, VMEM],
        out_specs=VMEM,
        out_shape=jax.ShapeDtypeStruct((rows, width), f32),
        scratch_shapes=[pltpu.VMEM((rows, width), bf16), pltpu.SemaphoreType.DMA],
        compiler_params=params(8),
        name="base",
    )(stay(shard), own_part, from_sib)
    pieces = 4
    result = pl.pallas_call(
        functools.partial(sum_kernel, n_chip - 1),
        in_specs=[SMEM, VMEM] + [HBM] * len(back),
        out_specs=HBM,
        out_shape=jax.ShapeDtypeStruct((rows, width), bf16),
        scratch_shapes=[
            pltpu.VMEM((n_chip - 1, rows, width), bf16),
            pltpu.SemaphoreType.DMA((n_chip - 1, pieces)),
            pltpu.SemaphoreType.DMA((pieces,)),
        ],
        compiler_params=params(10),
        name="sum",
    )(idx, base, *back)
    return (result[None], dec_out)


def solution(mesh):
    return jax.shard_map(
        layer,
        mesh=mesh,
        in_specs=(
            P(("pool", "batch"), "blk", None),
            P("pool", "batch"),
            P(None, ("pool", "batch"), None),
            P(("pool", "batch"), None, "blk"),
            P(("pool", "batch"), None, "blk"),
            P(("pool", "batch")),
            P("pool", "batch"),
            P("pool", "batch"),
            P(),
            P(None, "blk"),
            P("blk", None),
        ),
        out_specs=(P(("pool", "batch"), "blk", None), P(None, ("pool", "batch"), None)),
        check_vma=False,
    )
```

```python
import functools

import jax
import jax.numpy as jnp
import numpy as np
from jax import lax
from jax.experimental import pallas as pl
from jax.experimental.pallas import tpu as pltpu
from jax.sharding import PartitionSpec as P


HEAD_DIM = 128
GROUP = 4
KINDS = GROUP + 2
PAIR = 2 * HEAD_DIM
BLOCKS = KINDS // 2
EPSILON = 1e-05
THETA = 500000.0
NEG = -1e30
SCALE = HEAD_DIM ** (-0.5)
OUT_COLS = 1024
f32 = jnp.float32
bf16 = jnp.bfloat16


VMEM = pl.BlockSpec(memory_space=pltpu.MemorySpace.VMEM)
SMEM = pl.BlockSpec(memory_space=pltpu.MemorySpace.SMEM)
HBM = pl.BlockSpec(memory_space=pltpu.MemorySpace.HBM)
ANY = pl.BlockSpec(memory_space=pl.ANY)


def dot(a, b):
    return jnp.dot(a, b, preferred_element_type=f32)


def dot_t(a, b):
    return lax.dot_general(a, b, (((1,), (1,)), ((), ())), preferred_element_type=f32)


def rot(u, cosine, sine):
    return u * cosine + pltpu.roll(u, HEAD_DIM // 2, 1) * sine


def angle_tables(places):
    half = HEAD_DIM // 2
    freqs = THETA ** (-(jnp.arange(HEAD_DIM) % half).astype(f32) / half)
    angles = places.astype(f32)[..., None] * freqs
    first = jnp.arange(HEAD_DIM) < half
    return jnp.where(first, jnp.cos(angles), jnp.sin(angles))


def spread(table):
    half = HEAD_DIM // 2
    turned = pltpu.roll(table, half, 1)
    first = lax.broadcasted_iota(jnp.int32, table.shape, 1) < half
    return jnp.where(first, table, turned), jnp.where(first, -turned, table)


def fixed_tables(count):
    half = HEAD_DIM // 2
    freqs = np.float32(THETA) ** (-np.arange(half, dtype=np.float32) / np.float32(half))
    angles = np.arange(count, dtype=np.float32)[:, None] * freqs.astype(np.float32)
    cosine, sine = np.cos(angles).astype(np.float32), np.sin(angles).astype(np.float32)
    return np.concatenate([cosine, cosine], -1), np.concatenate([-sine, sine], -1)


def norm_rows(src, dst, offset, gain_ref):
    rows = src.shape[0]

    def step(i, _):
        at = pl.multiple_of(i * 16, 16)
        wide = src[pl.ds(at, 16), :].astype(f32)
        factor = lax.rsqrt(jnp.mean(wide * wide, axis=-1, keepdims=True) + EPSILON)
        to = pl.multiple_of(offset + i * 16, 16)
        dst[pl.ds(to, 16), :] = (wide * factor * gain_ref[...]).astype(bf16)
        return 0

    lax.fori_loop(0, rows // 16, step, 0, unroll=2)


def weight_copies(w_hbm, w_vmem, sems, width):
    return [
        pltpu.make_async_copy(
            w_hbm.at[:, pl.ds(j * width, width)], w_vmem.at[j], sems.at[j]
        )
        for j in range(w_vmem.shape[0])
    ]


def rotated_pair(acc, cosine, sine, j):
    cosine, sine = cosine[...], sine[...]
    first = rot(acc[:, :HEAD_DIM], cosine, sine)
    second = acc[:, HEAD_DIM:]
    if j % BLOCKS != BLOCKS - 1:
        second = rot(second, cosine, sine)
    return jnp.concatenate([first, second], axis=1).astype(bf16)


def load(pairs, sems):
    copies = [pltpu.make_async_copy(src, dst, sems.at[i]) for i, (src, dst) in enumerate(pairs)]
    for copy in copies:
        copy.start()
    return copies


def norm_token_rows(parts, gain_ref):
    out = []
    for part in parts:
        wide = part.astype(f32)
        factor = lax.rsqrt(jnp.mean(wide * wide, axis=-1, keepdims=True) + EPSILON)
        out.append(wide * factor * gain_ref[...])
    return jnp.concatenate(out, axis=0).astype(bf16)


def first_kernel(
    idx, slot, assign, own_hbm, dec_hbm, gain_hbm, cos_hbm, sin_hbm, wq_hbm,
    _, own_out, raw_out, wq, ask_out,
    own, dec, gain, tabs, normed, q_sems, in_sems,
):
    rows = own.shape[0]
    steps, decs = dec.shape[:2]
    at = pl.ds(pl.multiple_of(idx[0] * rows, rows), rows)
    weights = weight_copies(wq_hbm, wq, q_sems, PAIR)
    ready = load(
        [
            (gain_hbm, gain), (own_hbm, own), (dec_hbm, dec),
            (cos_hbm.at[at], tabs.at[0]), (sin_hbm.at[at], tabs.at[1]),
        ],
        in_sems,
    )
    weights[0].start()
    ready[0].wait()
    ready[1].wait()
    for copy in weights[1:4]:
        copy.start()
    norm_rows(own, normed, 0, gain)
    ready[2].wait()
    tokens = [dec[s].astype(f32) for s in range(steps)]
    normed[rows:] = norm_token_rows(tokens, gain)
    fresh = []
    for s in range(steps):
        row = tokens[s][:1]
        for r in range(1, decs):
            row = jnp.where(slot[0, 0] == r, tokens[s][r : r + 1], row)
        fresh.append(row)
    fresh.append(jnp.full((steps, dec.shape[2]), assign[0, 0].astype(f32)))
    ask_out[...] = jnp.concatenate(fresh, axis=0).astype(bf16)
    for copy in ready[3:]:
        copy.wait()
    for j in range(wq.shape[0]):
        weights[j].wait()
        if j + 4 < len(weights):
            weights[j + 4].start()
        acc = dot(normed[...], wq[j])
        own_out[j] = rotated_pair(acc[:rows], tabs.at[0], tabs.at[1], j)
        for r in range(decs):
            for s in range(steps):
                row = rows + s * decs + r
                raw_out[r, j, s : s + 1] = acc[row : row + 1]


def project_kernel(which, n_ask, *refs):
    refs = list(refs)
    take = lambda n: [refs.pop(0) for _ in range(n)]
    idx, x_hbm, gain_hbm, cos_hbm, sin_hbm, wq = take(6)
    asks = take(n_ask)
    out = take(1)[0]
    raw_out = take(1)[0] if n_ask else None
    x, gain, tabs, normed, in_sem = take(5)
    rows = x.shape[0]
    at = pl.ds(pl.multiple_of(idx[which] * rows, rows), rows)
    ready = load(
        [(gain_hbm, gain), (x_hbm, x), (cos_hbm.at[at], tabs.at[0]), (sin_hbm.at[at], tabs.at[1])],
        in_sem,
    )
    ready[0].wait()
    if n_ask:
        here = idx[idx.shape[0] - 1].astype(f32)
        steps = asks[0].shape[0] // 2
        new = jnp.zeros((steps, x.shape[1]), f32)
        for ref in asks:
            wide = ref[...].astype(f32)
            new = jnp.where(wide[steps : steps + 1] == here, wide[:steps], new)
        fill = jnp.zeros((16 - steps, x.shape[1]), f32)
        normed[rows:] = norm_token_rows([new, fill], gain)
    ready[1].wait()
    norm_rows(x, normed, 0, gain)
    for copy in ready[2:]:
        copy.wait()
    for j in range(wq.shape[0]):
        acc = dot(normed[...], wq[j])
        out[j] = rotated_pair(acc[:rows], tabs.at[0], tabs.at[1], j)
        if n_ask:
            raw_out[j] = acc[rows : rows + raw_out.shape[1]]


def own_tail(q, k_own, steps):
    s = dot_t(q, k_own) * SCALE
    at = lax.broadcasted_iota(jnp.int32, s.shape, 0)
    t = lax.broadcasted_iota(jnp.int32, s.shape, 1)
    return jnp.where(t <= lax.rem(at, steps), s, NEG)


def stacked_queries(raw, h, cosine, sine):
    parts = []
    for g in range(GROUP):
        block = raw(h * BLOCKS + g // 2)
        parts.append(rot(block[:, (g % 2) * HEAD_DIM : (g % 2 + 1) * HEAD_DIM], cosine, sine))
    return jnp.concatenate(parts, axis=0).astype(bf16)


def own_pair(raw, h, cosine, sine, pad):
    block = raw(h * BLOCKS + BLOCKS - 1)
    key = rot(block[:, :HEAD_DIM], cosine, sine)
    fill = jnp.zeros((pad - key.shape[0], HEAD_DIM), f32)
    key = jnp.concatenate([key, fill], axis=0).astype(bf16)
    value = jnp.concatenate([block[:, HEAD_DIM:], fill], axis=0).astype(bf16)
    return key, value


def decode_kernel(first, loads, *refs):
    refs = list(refs)
    take = lambda n: [refs.pop(0) for _ in range(n)]
    lens, slot, raw_ref, angle_ref, k_hbm, v_hbm = take(6)
    wo_hbm = take(1)[0] if loads else None
    out_ref = take(1)[0]
    wo = take(1)[0] if loads else None
    k_s, v_s, q_s, ko_s, vo_s, m_s, l_s, acc_s, k_sem, v_sem = take(10)
    o_sem = take(1)[0] if loads else None
    group = raw_ref.shape[0]
    n_rows, count, width = k_s.shape[:3]
    steps = raw_ref.shape[2]
    heads = k_s.shape[3] // HEAD_DIM
    many = GROUP * steps

    def copies(r, j):
        at = pl.ds(j * width, width)
        return (
            pltpu.make_async_copy(k_hbm.at[first + r, at], k_s.at[r, j], k_sem.at[r, j]),
            pltpu.make_async_copy(v_hbm.at[first + r, at], v_s.at[r, j], v_sem.at[r, j]),
        )

    def live(r, j):
        return (j * width < lens[first + r]) & (slot[0, 0] != first + r)

    def fetch(r):
        for j in range(count):

            @pl.when(live(r, j))
            def _(r=r, j=j):
                for copy in copies(r, j):
                    copy.start()

    weights = weight_copies(wo_hbm, wo, o_sem, OUT_COLS) if loads else []
    fetch(0)
    for r in range(n_rows):
        raw = lambda b, r=r: raw_ref[first + r, b]
        turn = spread(angle_ref[first + r])
        q_s[r] = jnp.zeros_like(q_s[r])
        for h in range(heads):
            lanes = slice(h * HEAD_DIM, (h + 1) * HEAD_DIM)
            q_s[r, h * many : (h + 1) * many, lanes] = stacked_queries(raw, h, *turn)
            key, value = own_pair(raw, h, *turn, ko_s.shape[1])
            ko_s[r, :, lanes] = key
            vo_s[r, :, lanes] = value
    for r in range(n_rows):
        s = own_tail(q_s[r], ko_s[r], steps)
        m = jnp.max(s, axis=-1, keepdims=True)
        e = jnp.exp(s - m)
        m_s[r] = m
        l_s[r] = jnp.sum(e, axis=-1, keepdims=True)
        acc_s[r] = dot(e.astype(bf16), vo_s[r])

    for r in range(n_rows):
        if r + 1 < n_rows:
            fetch(r + 1)
        for j in range(count):

            @pl.when(live(r, j))
            def _(r=r, j=j):
                k_copy, v_copy = copies(r, j)
                k_copy.wait()
                s = dot_t(q_s[r], k_s[r, j]) * SCALE
                at = j * width + lax.broadcasted_iota(jnp.int32, s.shape, 1)
                s = jnp.where(at < lens[first + r], s, NEG)
                m = jnp.maximum(m_s[r], jnp.max(s, axis=-1, keepdims=True))
                fade = jnp.exp(m_s[r] - m)
                e = jnp.exp(s - m)
                m_s[r] = m
                l_s[r] = l_s[r] * fade + jnp.sum(e, axis=-1, keepdims=True)
                v_copy.wait()
                acc_s[r] = acc_s[r] * fade + dot(e.astype(bf16), v_s[r, j])

        for copy in weights[r * len(weights) // n_rows : (r + 1) * len(weights) // n_rows]:
            copy.start()

    for r in range(n_rows):
        mixed = acc_s[r] / l_s[r]
        for h in range(heads):
            for g in range(GROUP):
                to = (h * GROUP + g) * HEAD_DIM
                for s in range(steps):
                    at = h * many + g * steps + s
                    row = s * group + first + r
                    out_ref[row : row + 1, to : to + HEAD_DIM] = mixed[
                        at : at + 1, h * HEAD_DIM : (h + 1) * HEAD_DIM
                    ]
    for copy in weights:
        copy.wait()


def attend(queries, q_shard, pieces, plen, out_ref, offset, heads):
    for h in range(heads):
        parts = []
        for g in range(GROUP):
            block = queries(h * BLOCKS + g // 2)
            parts.append(block[:, (g % 2) * HEAD_DIM : (g % 2 + 1) * HEAD_DIM])
        rows = parts[0].shape[0]
        q = jnp.concatenate(parts, axis=0)
        q_at = q_shard * rows + lax.rem(lax.broadcasted_iota(jnp.int32, (GROUP * rows, 1), 0), rows)
        scores, values = [], []
        for kv, shard in pieces:
            pair = kv(h)
            count = pair.shape[0]
            k_at = shard * count + lax.broadcasted_iota(jnp.int32, (1, count), 1)
            k_at = jnp.where(k_at < plen, k_at, jnp.int32(1 << 30))
            s = dot_t(q, pair[:, :HEAD_DIM]) * SCALE
            scores.append(jnp.where(k_at <= q_at, s, NEG))
            values.append(pair[:, HEAD_DIM:])
        top = functools.reduce(jnp.maximum, scores)
        top = jnp.max(top, axis=-1, keepdims=True)
        total, mixed = None, None
        for s, value in zip(scores, values):
            e = jnp.exp(s - top)
            total = e if total is None else total + e
            term = dot(e.astype(bf16), value)
            mixed = term if mixed is None else mixed + term
        mixed = (mixed / jnp.sum(total, axis=-1, keepdims=True)).astype(bf16)
        for g in range(GROUP):
            to = (h * GROUP + g) * HEAD_DIM
            out_ref[offset : offset + rows, to : to + HEAD_DIM] = mixed[g * rows : (g + 1) * rows]


def attend_new(raw, cosine, sine, pieces, plen, out_ref, heads, steps):
    spread = out_ref.shape[0] // steps
    for h in range(heads):
        q = stacked_queries(raw, h, cosine, sine)
        key, value = own_pair(raw, h, cosine, sine, 16)
        scores, values = [own_tail(q, key, steps)], [value]
        for kv, shard in pieces:
            pair = kv(h)
            count = pair.shape[0]
            k_at = shard * count + lax.broadcasted_iota(jnp.int32, (1, count), 1)
            s = dot_t(q, pair[:, :HEAD_DIM]) * SCALE
            scores.append(jnp.where(k_at < plen, s, NEG))
            values.append(pair[:, HEAD_DIM:])
        top = functools.reduce(jnp.maximum, [jnp.max(s, axis=-1, keepdims=True) for s in scores])
        total, mixed = 0.0, 0.0
        for s, v in zip(scores, values):
            e = jnp.exp(s - top)
            total = total + jnp.sum(e, axis=-1, keepdims=True)
            mixed = mixed + dot(e.astype(bf16), v)
        mixed = mixed / total
        for g in range(GROUP):
            to = (h * GROUP + g) * HEAD_DIM
            rows = [
                jnp.broadcast_to(mixed[g * steps + s : g * steps + s + 1], (spread, HEAD_DIM))
                for s in range(steps)
            ]
            out_ref[:, to : to + HEAD_DIM] = jnp.concatenate(rows, axis=0).astype(bf16)


def chunk_kernel(which, n_full, n_kv, n_ask, kv_only, *refs):
    refs = list(refs)
    take = lambda n: [refs.pop(0) for _ in range(n)]
    idx, plen, passed, gain_hbm, cos_hbm, sin_hbm, direct, wq, wo = take(9)
    full, kvs = take(n_full), take(n_kv)
    raw_s, new_angle = take(2) if n_ask else (None, None)
    kv_out = take(1)[0]
    direct_out, passed_out = (None,) * 2 if kv_only else take(2)
    new_out = take(1)[0] if n_ask else None
    x, gain, tabs, normed, qkv, in_sem = take(6)
    attn = None if kv_only else take(1)[0]
    rows = x.shape[0]
    heads = kv_out.shape[0] // 2
    shards = [idx[n_full + 2 * which + i] for i in range(2)]
    at = pl.ds(pl.multiple_of(shards[1] * rows, rows), rows)
    ready = load(
        [(gain_hbm, gain), (passed, x), (cos_hbm.at[at], tabs.at[0]), (sin_hbm.at[at], tabs.at[1])],
        in_sem,
    )
    ready[0].wait()
    ready[1].wait()
    norm_rows(x, normed, 0, gain)
    for copy in ready[2:]:
        copy.wait()
    for j in range(wq.shape[0]):
        qkv[j] = rotated_pair(dot(normed[...], wq[j]), tabs.at[0], tabs.at[1], j)
    both = (direct, qkv)
    for i in range(2):
        for h in range(heads):
            kv_out[i * heads + h] = both[i][h * BLOCKS + BLOCKS - 1]
    if kv_only:
        return
    pieces = [(lambda h, ref=ref: ref[h * BLOCKS + BLOCKS - 1], idx[i]) for i, ref in enumerate(full)]
    others = [n for n in range(n_kv + 1) if n != which]
    for ref, n in zip(kvs, others):
        for i in range(2):
            pieces.append((lambda h, ref=ref, i=i: ref[i * heads + h], idx[n_full + 2 * n + i]))
    for i in range(2):
        pieces.append((lambda h, i=i: both[i][h * BLOCKS + BLOCKS - 1], shards[i]))
    for i in (1, 0):
        attend(lambda b, i=i: both[i][b], shards[i], pieces, plen[0, 0], attn, i * rows, heads)
    if n_ask:
        steps = new_angle.shape[0]
        raw = lambda b: raw_s[b, :steps]
        attend_new(raw, *spread(new_angle[...]), pieces, plen[0, 0], new_out, heads, steps)
    for j in range(wo.shape[0]):
        cols = slice(j * OUT_COLS, (j + 1) * OUT_COLS)
        part = dot(attn[...], wo[j]).astype(bf16)
        direct_out[:, cols] = part[:rows]
        passed_out[:, cols] = part[rows:]


def last_kernel(n_kv, n_ret, n_rows, *refs):
    refs = list(refs)
    take = lambda n: [refs.pop(0) for _ in range(n)]
    idx, plen, slot, assign, own, sib = take(6)
    kvs = take(n_kv)
    decs = take(2)
    rets = take(n_ret)
    wo, own_part, sib_part, dec_part, attn = take(5)
    rows = own.shape[1]
    heads = kvs[0].shape[0] // 2
    pieces = [(lambda h, ref=ref: ref[h * BLOCKS + BLOCKS - 1], idx[i]) for i, ref in enumerate((own, sib))]
    for n, ref in enumerate(kvs):
        for i in range(2):
            pieces.append((lambda h, ref=ref, i=i: ref[i * heads + h], idx[2 + 2 * n + i]))
    for i, ref in enumerate((own, sib)):
        attend(lambda b, ref=ref: ref[b], idx[i], pieces, plen[0, 0], attn, i * rows, heads)
    pick = lax.rem(idx[idx.shape[0] - 1] - assign[0, 0] + n_ret, n_ret)
    new = rets[0][...].astype(f32)
    for k in range(1, n_ret):
        new = jnp.where(pick == k, rets[k][...].astype(f32), new)
    at = lax.rem(lax.broadcasted_iota(jnp.int32, new.shape, 0), n_rows)
    dec = jnp.where(at < n_rows // 2, decs[0][...], decs[1][...])
    attn[2 * rows :] = jnp.where(at == slot[0, 0], new, dec).astype(bf16)
    for j in range(wo.shape[0]):
        part = dot(attn[...], wo[j]).astype(bf16)
        cols = slice(j * OUT_COLS, (j + 1) * OUT_COLS)
        own_part[:, cols] = part[:rows]
        sib_part[:, cols] = part[rows:]
        dec_part[:, cols] = part[2 * rows :]


def add_kernel(start, a, b, out):
    rows = out.shape[0]

    def step(i, _):
        at = pl.ds(pl.multiple_of(i * 16, 16), 16)
        to = pl.ds(pl.multiple_of(start + i * 16, 16), 16)
        out[at, :] = (a[at, :].astype(f32) + b[to, :].astype(f32)).astype(bf16)
        return 0

    lax.fori_loop(0, rows // 16, step, 0)


def base_kernel(shard_hbm, own, sib, out, shard, sem):
    copy = pltpu.make_async_copy(shard_hbm, shard, sem)
    copy.start()
    copy.wait()

    def step(i, _):
        at = pl.ds(pl.multiple_of(i * 16, 16), 16)
        out[at, :] = shard[at, :].astype(f32) + own[at, :].astype(f32) + sib[at, :].astype(f32)
        return 0

    lax.fori_loop(0, out.shape[0] // 16, step, 0)


def sum_kernel(count, base, *refs):
    parts, out, got, sems, out_sem = refs[:count], *refs[count:]
    pieces = sems.shape[1]
    rows = out.shape[0] // pieces
    copies = [
        [
            pltpu.make_async_copy(parts[d].at[pl.ds(n * rows, rows)], got.at[d, pl.ds(n * rows, rows)], sems.at[d, n])
            for d in range(count)
        ]
        for n in range(pieces)
    ]
    for copy in sum(copies, []):
        copy.start()
    done = []
    for n in range(pieces):
        at = slice(n * rows, (n + 1) * rows)
        total = base[at]
        for d in range(count):
            copies[n][d].wait()
            total = total + got[d, at].astype(f32)
        got[0, at] = total.astype(bf16)
        done.append(pltpu.make_async_copy(got.at[0, pl.ds(n * rows, rows)], out.at[pl.ds(n * rows, rows)], out_sem.at[n]))
        done[-1].start()
    for copy in done:
        copy.wait()


def dec_kernel(tokens, a, b, out):
    steps, n_rows = tokens.shape[:2]
    total = a[...].astype(f32) + b[...].astype(f32)
    for s in range(steps):
        rows = total[s * n_rows : (s + 1) * n_rows]
        out[s] = (tokens[s].astype(f32) + rows).astype(bf16)


def params(mib):
    return pltpu.CompilerParams(vmem_limit_bytes=mib << 20)


def layer(
    prompt, prompt_len, dec_tokens, cache_k, cache_v, cache_len, assign, slot, gain, w_qkv, w_out
):
    n_blk, n_pool, n_batch = lax.axis_size("blk"), lax.axis_size("pool"), lax.axis_size("batch")
    n_chip = n_blk // 2
    shard = prompt[0]
    rows, width = shard.shape
    steps, n_rows = dec_tokens.shape[:2]
    heads = w_qkv.shape[1] // (KINDS * HEAD_DIM)
    blocks = heads * BLOCKS
    attn_cols = heads * GROUP * HEAD_DIM
    out_blocks = width // OUT_COLS
    decs = steps * n_rows

    blk = lax.axis_index("blk")
    chip, core = blk // 2, blk % 2
    batch = lax.axis_index("batch")
    at = jnp.arange(n_blk + 1, dtype=jnp.int32)
    far = (chip + n_chip - at // 2) % n_chip
    idx = jnp.where(at == n_blk, batch, 2 * far + (core + at) % 2).astype(jnp.int32)
    gain_row = gain.reshape(1, width)
    cos_t, sin_t = (jnp.asarray(t) for t in fixed_tables(n_blk * rows))
    place = jnp.concatenate([cache_len, prompt_len[0]])[:, None]
    angles = angle_tables(place + jnp.arange(steps, dtype=jnp.int32)[None, :])
    dec_angle, new_angle = angles[:n_rows], angles[n_rows]

    swap = [(i, i ^ 1) for i in range(n_blk)]
    hop = lambda d: [(2 * c + k, 2 * ((c + d) % n_chip) + k) for c in range(n_chip) for k in range(2)]
    shift = [
        [
            (p * n_batch + b, ((p + n_pool // 2) % n_pool) * n_batch + (b + k) % n_batch)
            for p in range(n_pool)
            for b in range(n_batch)
        ]
        for k in range(n_batch)
    ]
    groups = ("pool", "batch")
    near = lambda x: pltpu.with_memory_space_constraint(x, pltpu.MemorySpace.VMEM)
    stay = lambda x: pltpu.with_memory_space_constraint(x, pltpu.MemorySpace.HBM)

    sib_x = lax.ppermute(shard, "blk", swap)
    far_x = []
    for d in range(1, n_chip):
        far_x.append(lax.ppermute(shard, "blk", hop(d)))

    own, raw, wq, ask = pl.pallas_call(
        first_kernel,
        in_specs=[SMEM] * 3 + [HBM] * 6 + [ANY],
        out_specs=[VMEM] * 4,
        out_shape=[
            jax.ShapeDtypeStruct((blocks, rows, PAIR), bf16),
            jax.ShapeDtypeStruct((n_rows, blocks, steps, PAIR), f32),
            pltpu.VMEM((blocks, width, PAIR), bf16),
            jax.ShapeDtypeStruct((2 * steps, width), bf16),
        ],
        scratch_shapes=[
            pltpu.VMEM((rows, width), bf16),
            pltpu.VMEM((steps, n_rows, width), bf16),
            pltpu.VMEM((1, width), f32),
            pltpu.VMEM((2, rows, HEAD_DIM), f32),
            pltpu.VMEM((rows + decs, width), bf16),
            pltpu.SemaphoreType.DMA((blocks,)),
            pltpu.SemaphoreType.DMA((5,)),
        ],
        compiler_params=params(8),
        name="first",
    )(
        idx, slot, assign, stay(shard), stay(dec_tokens), stay(gain_row), stay(cos_t),
        stay(sin_t), stay(w_qkv), angles,
    )

    def project(which, x, asks):
        outs = [jax.ShapeDtypeStruct((blocks, rows, PAIR), bf16)]
        if asks:
            outs.append(jax.ShapeDtypeStruct((blocks, 8, PAIR), f32))
        return pl.pallas_call(
            functools.partial(project_kernel, which, len(asks)),
            in_specs=[SMEM] + [HBM] * 4 + [VMEM] * (1 + len(asks)),
            out_specs=[VMEM] * len(outs),
            out_shape=outs,
            scratch_shapes=[
                pltpu.VMEM((rows, width), bf16),
                pltpu.VMEM((1, width), f32),
                pltpu.VMEM((2, rows, HEAD_DIM), f32),
                pltpu.VMEM((rows + (16 if asks else 0), width), bf16),
                pltpu.SemaphoreType.DMA((4,)),
            ],
            compiler_params=params(8),
            name="project",
        )(idx, x, stay(gain_row), stay(cos_t), stay(sin_t), near(wq), *asks)

    sib = project(1, sib_x, [])[0]
    asks = [lax.ppermute(ask, groups, perm) for perm in shift]

    cached = cache_k.shape[1]
    step_rows = min(2048, cached)
    count = cached // step_rows
    kv_width = heads * HEAD_DIM
    many = GROUP * steps * heads
    half_rows = n_rows // 2

    def decode(part):
        loads = part == 0
        return pl.pallas_call(
            functools.partial(decode_kernel, part * half_rows, loads),
            in_specs=[SMEM] * 2 + [VMEM] * 2 + [HBM] * (3 if loads else 2),
            out_specs=[VMEM] * (2 if loads else 1),
            out_shape=[
                jax.ShapeDtypeStruct((decs, attn_cols), f32),
                pltpu.VMEM((out_blocks, attn_cols, OUT_COLS), bf16),
            ][: 2 if loads else 1],
            scratch_shapes=[
                pltpu.VMEM((half_rows, count, step_rows, kv_width), bf16),
                pltpu.VMEM((half_rows, count, step_rows, kv_width), bf16),
                pltpu.VMEM((half_rows, many, kv_width), bf16),
                pltpu.VMEM((half_rows, 16, kv_width), bf16),
                pltpu.VMEM((half_rows, 16, kv_width), bf16),
                pltpu.VMEM((half_rows, many, 1), f32),
                pltpu.VMEM((half_rows, many, 1), f32),
                pltpu.VMEM((half_rows, many, kv_width), f32),
                pltpu.SemaphoreType.DMA((half_rows, count)),
                pltpu.SemaphoreType.DMA((half_rows, count)),
            ] + ([pltpu.SemaphoreType.DMA((out_blocks,))] if loads else []),
            compiler_params=params(12),
            name="decode",
        )(
            cache_len, slot, raw, dec_angle, stay(cache_k), stay(cache_v),
            *([stay(w_out)] if loads else []),
        )

    dec_low, wo = decode(0)
    dec_high = decode(1)[0]

    def chunk(n, kvs, asks, kv_only):
        passed = lax.ppermute(far_x[n], "blk", swap)
        direct, *news = project(2 + 2 * n, far_x[n], asks)
        outs = [jax.ShapeDtypeStruct((2 * heads, rows, PAIR), bf16)]
        scratch = [
            pltpu.VMEM((rows, width), bf16),
            pltpu.VMEM((1, width), f32),
            pltpu.VMEM((2, rows, HEAD_DIM), f32),
            pltpu.VMEM((rows, width), bf16),
            pltpu.VMEM((blocks, rows, PAIR), bf16),
            pltpu.SemaphoreType.DMA((4,)),
        ]
        if not kv_only:
            outs += [jax.ShapeDtypeStruct((rows, width), bf16)] * 2
            scratch.append(pltpu.VMEM((2 * rows, attn_cols), bf16))
        extra = []
        if asks:
            outs.append(jax.ShapeDtypeStruct((decs, attn_cols), bf16))
            extra = [*news, new_angle]
        kernel = functools.partial(chunk_kernel, n, 2, len(kvs), len(asks), kv_only)
        return pl.pallas_call(
            kernel,
            in_specs=[SMEM] * 2 + [HBM] * 4 + [VMEM] * (5 + len(kvs) + len(extra)),
            out_specs=[VMEM] * len(outs),
            out_shape=outs,
            scratch_shapes=scratch,
            compiler_params=params(16),
            name="chunk",
        )(
            idx, prompt_len, passed, stay(gain_row), stay(cos_t), stay(sin_t),
            direct, near(wq), near(wo), own, sib, *kvs, *extra,
        )

    def add(a, b, start=0):
        return pl.pallas_call(
            functools.partial(add_kernel, start),
            in_specs=[VMEM] * 2,
            out_specs=VMEM,
            out_shape=jax.ShapeDtypeStruct(a.shape, bf16),
            compiler_params=params(8),
            name="add",
        )(a, b)

    kvs, back, fresh = [], [], None
    ahead = n_chip > 2
    if ahead:
        kvs = [chunk(n, [], [], True)[0] for n in range(n_chip - 1)]
    for n in range(n_chip - 1):
        final = n == n_chip - 2
        others = [kv for i, kv in enumerate(kvs) if i != n]
        outs = chunk(n, others, asks if final else [], False)
        if not ahead:
            kvs.append(outs[0])
        if final:
            fresh = outs[3]
        other = lax.ppermute(outs[2], "blk", swap)
        both = add(outs[1], other)
        back.append(lax.ppermute(both, "blk", hop(n_chip - 1 - n)))

    rets = [lax.ppermute(fresh, groups, perm) for perm in shift]
    own_part, sib_part, dec_part = pl.pallas_call(
        functools.partial(last_kernel, len(kvs), n_batch, n_rows),
        in_specs=[SMEM] * 4 + [VMEM] * (5 + len(kvs) + n_batch),
        out_specs=[VMEM] * 3,
        out_shape=[
            jax.ShapeDtypeStruct((rows, width), bf16),
            jax.ShapeDtypeStruct((rows + decs, width), bf16),
            jax.ShapeDtypeStruct((decs, width), bf16),
        ],
        scratch_shapes=[
            pltpu.VMEM((2 * rows + decs, attn_cols), bf16),
        ],
        compiler_params=params(12),
        name="last",
    )(idx, prompt_len, slot, assign, own, sib, *kvs, dec_low, dec_high, *rets, near(wo))
    from_sib = lax.ppermute(sib_part, "blk", swap)

    total = add(dec_part, from_sib, rows)
    reach = 1
    while reach < n_chip:
        other = lax.ppermute(total, "blk", [(i, i ^ (2 * reach)) for i in range(n_blk)])
        reach *= 2
        if reach < n_chip:
            total = add(total, other)
    dec_out = pl.pallas_call(
        dec_kernel,
        in_specs=[VMEM] * 3,
        out_specs=VMEM,
        out_shape=jax.ShapeDtypeStruct(dec_tokens.shape, bf16),
        compiler_params=params(8),
        name="dec",
    )(dec_tokens, total, other)
    base = pl.pallas_call(
        base_kernel,
        in_specs=[HBM, VMEM, VMEM],
        out_specs=VMEM,
        out_shape=jax.ShapeDtypeStruct((rows, width), f32),
        scratch_shapes=[pltpu.VMEM((rows, width), bf16), pltpu.SemaphoreType.DMA],
        compiler_params=params(8),
        name="base",
    )(stay(shard), own_part, from_sib)
    pieces = 4
    result = pl.pallas_call(
        functools.partial(sum_kernel, n_chip - 1),
        in_specs=[VMEM] + [HBM] * len(back),
        out_specs=HBM,
        out_shape=jax.ShapeDtypeStruct((rows, width), bf16),
        scratch_shapes=[
            pltpu.VMEM((n_chip - 1, rows, width), bf16),
            pltpu.SemaphoreType.DMA((n_chip - 1, pieces)),
            pltpu.SemaphoreType.DMA((pieces,)),
        ],
        compiler_params=params(10),
        name="sum",
    )(base, *back)
    return (result[None], dec_out)


def solution(mesh):
    return jax.shard_map(
        layer,
        mesh=mesh,
        in_specs=(
            P(("pool", "batch"), "blk", None),
            P("pool", "batch"),
            P(None, ("pool", "batch"), None),
            P(("pool", "batch"), None, "blk"),
            P(("pool", "batch"), None, "blk"),
            P(("pool", "batch")),
            P("pool", "batch"),
            P("pool", "batch"),
            P(),
            P(None, "blk"),
            P("blk", None),
        ),
        out_specs=(P(("pool", "batch"), "blk", None), P(None, ("pool", "batch"), None)),
        check_vma=False,
    )
```

```python
import functools

import jax
import jax.numpy as jnp
import numpy as np
from jax import lax
from jax.experimental import pallas as pl
from jax.experimental.pallas import tpu as pltpu
from jax.sharding import PartitionSpec as P


HEAD_DIM = 128
GROUP = 4
KINDS = GROUP + 2
PAIR = 2 * HEAD_DIM
BLOCKS = KINDS // 2
EPSILON = 1e-05
THETA = 500000.0
NEG = -1e30
SCALE = HEAD_DIM ** (-0.5)
OUT_COLS = 1024
f32 = jnp.float32
bf16 = jnp.bfloat16


VMEM = pl.BlockSpec(memory_space=pltpu.MemorySpace.VMEM)
SMEM = pl.BlockSpec(memory_space=pltpu.MemorySpace.SMEM)
HBM = pl.BlockSpec(memory_space=pltpu.MemorySpace.HBM)
ANY = pl.BlockSpec(memory_space=pl.ANY)


def dot(a, b):
    return jnp.dot(a, b, preferred_element_type=f32)


def dot_t(a, b):
    return lax.dot_general(a, b, (((1,), (1,)), ((), ())), preferred_element_type=f32)


def rot(u, cosine, sine):
    return u * cosine + pltpu.roll(u, HEAD_DIM // 2, 1) * sine


def angle_tables(places):
    half = HEAD_DIM // 2
    freqs = THETA ** (-(jnp.arange(HEAD_DIM) % half).astype(f32) / half)
    angles = places.astype(f32)[..., None] * freqs
    first = jnp.arange(HEAD_DIM) < half
    return jnp.where(first, jnp.cos(angles), jnp.sin(angles))


def spread(table):
    half = HEAD_DIM // 2
    turned = pltpu.roll(table, half, 1)
    first = lax.broadcasted_iota(jnp.int32, table.shape, 1) < half
    return jnp.where(first, table, turned), jnp.where(first, -turned, table)


def fixed_tables(count):
    half = HEAD_DIM // 2
    freqs = np.float32(THETA) ** (-np.arange(half, dtype=np.float32) / np.float32(half))
    angles = np.arange(count, dtype=np.float32)[:, None] * freqs.astype(np.float32)
    cosine, sine = np.cos(angles).astype(np.float32), np.sin(angles).astype(np.float32)
    return np.concatenate([cosine, cosine], -1), np.concatenate([-sine, sine], -1)


def norm_rows(src, dst, offset, gain_ref):
    rows = src.shape[0]

    def step(i, _):
        at = pl.multiple_of(i * 16, 16)
        wide = src[pl.ds(at, 16), :].astype(f32)
        factor = lax.rsqrt(jnp.mean(wide * wide, axis=-1, keepdims=True) + EPSILON)
        to = pl.multiple_of(offset + i * 16, 16)
        dst[pl.ds(to, 16), :] = (wide * factor * gain_ref[...]).astype(bf16)
        return 0

    lax.fori_loop(0, rows // 16, step, 0, unroll=2)


def weight_copies(w_hbm, w_vmem, sems, width):
    return [
        pltpu.make_async_copy(
            w_hbm.at[:, pl.ds(j * width, width)], w_vmem.at[j], sems.at[j]
        )
        for j in range(w_vmem.shape[0])
    ]


def rotated_pair(acc, cosine, sine, j):
    cosine, sine = cosine[...], sine[...]
    first = rot(acc[:, :HEAD_DIM], cosine, sine)
    second = acc[:, HEAD_DIM:]
    if j % BLOCKS != BLOCKS - 1:
        second = rot(second, cosine, sine)
    return jnp.concatenate([first, second], axis=1).astype(bf16)


def load(pairs, sems):
    copies = [pltpu.make_async_copy(src, dst, sems.at[i]) for i, (src, dst) in enumerate(pairs)]
    for copy in copies:
        copy.start()
    return copies


def norm_token_rows(parts, gain_ref):
    out = []
    for part in parts:
        wide = part.astype(f32)
        factor = lax.rsqrt(jnp.mean(wide * wide, axis=-1, keepdims=True) + EPSILON)
        out.append(wide * factor * gain_ref[...])
    return jnp.concatenate(out, axis=0).astype(bf16)


def first_kernel(
    idx, slot, assign, own_hbm, sib_hbm, dec_hbm, gain_hbm, cos_hbm, sin_hbm, wq_hbm,
    _a, _b, own_out, sib_out, raw_out, wq, ask_out,
    own, sib, dec, gain, tabs, normed, q_sems, in_sems,
):
    rows = own.shape[0]
    steps, decs = dec.shape[:2]
    weights = weight_copies(wq_hbm, wq, q_sems, PAIR)
    ready = load([(gain_hbm, gain), (own_hbm, own), (dec_hbm, dec), (sib_hbm, sib)], in_sems)
    weights[0].start()
    for i in range(2):
        at = pl.ds(pl.multiple_of(idx[i] * rows, rows), rows)
        ready += load(
            [(cos_hbm.at[at], tabs.at[2 * i]), (sin_hbm.at[at], tabs.at[2 * i + 1])],
            in_sems.at[pl.ds(4 + 2 * i, 2)],
        )
    ready[0].wait()
    ready[1].wait()
    for copy in weights[1:4]:
        copy.start()
    norm_rows(own, normed, 0, gain)
    ready[2].wait()
    tokens = [dec[s].astype(f32) for s in range(steps)]
    normed[2 * rows :] = norm_token_rows(tokens, gain)
    fresh = []
    for s in range(steps):
        row = tokens[s][:1]
        for r in range(1, decs):
            row = jnp.where(slot[0, 0] == r, tokens[s][r : r + 1], row)
        fresh.append(row)
    fresh.append(jnp.full((steps, dec.shape[2]), assign[0, 0].astype(f32)))
    ask_out[...] = jnp.concatenate(fresh, axis=0).astype(bf16)
    ready[3].wait()
    norm_rows(sib, normed, rows, gain)
    for copy in ready[4:]:
        copy.wait()
    for j in range(wq.shape[0]):
        weights[j].wait()
        if j + 4 < len(weights):
            weights[j + 4].start()
        acc = dot(normed[...], wq[j])
        own_out[j] = rotated_pair(acc[:rows], tabs.at[0], tabs.at[1], j)
        sib_out[j] = rotated_pair(acc[rows : 2 * rows], tabs.at[2], tabs.at[3], j)
        for r in range(decs):
            for s in range(steps):
                row = 2 * rows + s * decs + r
                raw_out[r, j, s : s + 1] = acc[row : row + 1]


def project_kernel(which, loads, *refs):
    refs = list(refs)
    take = lambda n: [refs.pop(0) for _ in range(n)]
    idx, x_hbm, gain_hbm, cos_hbm, sin_hbm, wq = take(6)
    wo_hbm = take(1)[0] if loads else None
    out = take(1)[0]
    wo = take(1)[0] if loads else None
    x, gain, tabs, normed, in_sem = take(5)
    weights = weight_copies(wo_hbm, wo, take(1)[0], OUT_COLS) if loads else []
    rows = x.shape[0]
    at = pl.ds(pl.multiple_of(idx[which] * rows, rows), rows)
    ready = load(
        [(gain_hbm, gain), (x_hbm, x), (cos_hbm.at[at], tabs.at[0]), (sin_hbm.at[at], tabs.at[1])],
        in_sem,
    )
    ready[0].wait()
    ready[1].wait()
    for copy in weights:
        copy.start()
    norm_rows(x, normed, 0, gain)
    for copy in ready[2:]:
        copy.wait()
    for j in range(wq.shape[0]):
        out[j] = rotated_pair(dot(normed[...], wq[j]), tabs.at[0], tabs.at[1], j)
    for copy in weights:
        copy.wait()


def own_tail(q, k_own, steps):
    s = dot_t(q, k_own) * SCALE
    at = lax.broadcasted_iota(jnp.int32, s.shape, 0)
    t = lax.broadcasted_iota(jnp.int32, s.shape, 1)
    return jnp.where(t <= lax.rem(at, steps), s, NEG)


def stacked_queries(raw, h, cosine, sine):
    parts = []
    for g in range(GROUP):
        block = raw(h * BLOCKS + g // 2)
        parts.append(rot(block[:, (g % 2) * HEAD_DIM : (g % 2 + 1) * HEAD_DIM], cosine, sine))
    return jnp.concatenate(parts, axis=0).astype(bf16)


def own_pair(raw, h, cosine, sine, pad):
    block = raw(h * BLOCKS + BLOCKS - 1)
    key = rot(block[:, :HEAD_DIM], cosine, sine)
    fill = jnp.zeros((pad - key.shape[0], HEAD_DIM), f32)
    key = jnp.concatenate([key, fill], axis=0).astype(bf16)
    value = jnp.concatenate([block[:, HEAD_DIM:], fill], axis=0).astype(bf16)
    return key, value


def decode_kernel(first, *refs):
    refs = list(refs)
    take = lambda n: [refs.pop(0) for _ in range(n)]
    lens, slot, raw_ref, angle_ref, k_hbm, v_hbm = take(6)
    out_ref = take(1)[0]
    k_s, v_s, q_s, ko_s, vo_s, m_s, l_s, acc_s, k_sem, v_sem = take(10)
    group = raw_ref.shape[0]
    n_rows, count, width = k_s.shape[:3]
    steps = raw_ref.shape[2]
    heads = k_s.shape[3] // HEAD_DIM
    many = GROUP * steps

    def copies(r, j):
        at = pl.ds(j * width, width)
        return (
            pltpu.make_async_copy(k_hbm.at[first + r, at], k_s.at[r, j], k_sem.at[r, j]),
            pltpu.make_async_copy(v_hbm.at[first + r, at], v_s.at[r, j], v_sem.at[r, j]),
        )

    def live(r, j):
        return (j * width < lens[first + r]) & (slot[0, 0] != first + r)

    def fetch(r):
        for j in range(count):

            @pl.when(live(r, j))
            def _(r=r, j=j):
                for copy in copies(r, j):
                    copy.start()

    fetch(0)
    for r in range(n_rows):
        raw = lambda b, r=r: raw_ref[first + r, b]
        turn = spread(angle_ref[first + r])
        q_s[r] = jnp.zeros_like(q_s[r])
        for h in range(heads):
            lanes = slice(h * HEAD_DIM, (h + 1) * HEAD_DIM)
            q_s[r, h * many : (h + 1) * many, lanes] = stacked_queries(raw, h, *turn)
            key, value = own_pair(raw, h, *turn, ko_s.shape[1])
            ko_s[r, :, lanes] = key
            vo_s[r, :, lanes] = value
    for r in range(n_rows):
        s = own_tail(q_s[r], ko_s[r], steps)
        m = jnp.max(s, axis=-1, keepdims=True)
        e = jnp.exp(s - m)
        m_s[r] = m
        l_s[r] = jnp.sum(e, axis=-1, keepdims=True)
        acc_s[r] = dot(e.astype(bf16), vo_s[r])

    for r in range(n_rows):
        if r + 1 < n_rows:
            fetch(r + 1)
        for j in range(count):

            @pl.when(live(r, j))
            def _(r=r, j=j):
                k_copy, v_copy = copies(r, j)
                k_copy.wait()
                s = dot_t(q_s[r], k_s[r, j]) * SCALE
                at = j * width + lax.broadcasted_iota(jnp.int32, s.shape, 1)
                s = jnp.where(at < lens[first + r], s, NEG)
                m = jnp.maximum(m_s[r], jnp.max(s, axis=-1, keepdims=True))
                fade = jnp.exp(m_s[r] - m)
                e = jnp.exp(s - m)
                m_s[r] = m
                l_s[r] = l_s[r] * fade + jnp.sum(e, axis=-1, keepdims=True)
                v_copy.wait()
                acc_s[r] = acc_s[r] * fade + dot(e.astype(bf16), v_s[r, j])

    for r in range(n_rows):
        mixed = acc_s[r] / l_s[r]
        for h in range(heads):
            for g in range(GROUP):
                to = (h * GROUP + g) * HEAD_DIM
                for s in range(steps):
                    at = h * many + g * steps + s
                    row = s * group + first + r
                    out_ref[row : row + 1, to : to + HEAD_DIM] = mixed[
                        at : at + 1, h * HEAD_DIM : (h + 1) * HEAD_DIM
                    ]


def attend(queries, q_shard, pieces, plen, out_ref, offset, heads):
    for h in range(heads):
        parts = []
        for g in range(GROUP):
            block = queries(h * BLOCKS + g // 2)
            parts.append(block[:, (g % 2) * HEAD_DIM : (g % 2 + 1) * HEAD_DIM])
        rows = parts[0].shape[0]
        q = jnp.concatenate(parts, axis=0)
        q_at = q_shard * rows + lax.rem(lax.broadcasted_iota(jnp.int32, (GROUP * rows, 1), 0), rows)
        scores, values = [], []
        for kv, shard in pieces:
            pair = kv(h)
            count = pair.shape[0]
            k_at = shard * count + lax.broadcasted_iota(jnp.int32, (1, count), 1)
            k_at = jnp.where(k_at < plen, k_at, jnp.int32(1 << 30))
            s = dot_t(q, pair[:, :HEAD_DIM]) * SCALE
            scores.append(jnp.where(k_at <= q_at, s, NEG))
            values.append(pair[:, HEAD_DIM:])
        top = functools.reduce(jnp.maximum, scores)
        top = jnp.max(top, axis=-1, keepdims=True)
        total, mixed = None, None
        for s, value in zip(scores, values):
            e = jnp.exp(s - top)
            total = e if total is None else total + e
            term = dot(e.astype(bf16), value)
            mixed = term if mixed is None else mixed + term
        mixed = (mixed / jnp.sum(total, axis=-1, keepdims=True)).astype(bf16)
        for g in range(GROUP):
            to = (h * GROUP + g) * HEAD_DIM
            out_ref[offset : offset + rows, to : to + HEAD_DIM] = mixed[g * rows : (g + 1) * rows]


def attend_new(raw, cosine, sine, pieces, plen, out_ref, heads, steps):
    spread = out_ref.shape[0] // steps
    for h in range(heads):
        q = stacked_queries(raw, h, cosine, sine)
        key, value = own_pair(raw, h, cosine, sine, 16)
        scores, values = [own_tail(q, key, steps)], [value]
        for kv, shard in pieces:
            pair = kv(h)
            count = pair.shape[0]
            k_at = shard * count + lax.broadcasted_iota(jnp.int32, (1, count), 1)
            s = dot_t(q, pair[:, :HEAD_DIM]) * SCALE
            scores.append(jnp.where(k_at < plen, s, NEG))
            values.append(pair[:, HEAD_DIM:])
        top = functools.reduce(jnp.maximum, [jnp.max(s, axis=-1, keepdims=True) for s in scores])
        total, mixed = 0.0, 0.0
        for s, v in zip(scores, values):
            e = jnp.exp(s - top)
            total = total + jnp.sum(e, axis=-1, keepdims=True)
            mixed = mixed + dot(e.astype(bf16), v)
        mixed = mixed / total
        for g in range(GROUP):
            to = (h * GROUP + g) * HEAD_DIM
            rows = [
                jnp.broadcast_to(mixed[g * steps + s : g * steps + s + 1], (spread, HEAD_DIM))
                for s in range(steps)
            ]
            out_ref[:, to : to + HEAD_DIM] = jnp.concatenate(rows, axis=0).astype(bf16)


def chunk_kernel(which, n_full, n_kv, n_ask, kv_only, *refs):
    refs = list(refs)
    take = lambda n: [refs.pop(0) for _ in range(n)]
    idx, plen, passed, gain_hbm, cos_hbm, sin_hbm, direct, wq, wo = take(9)
    full, kvs = take(n_full), take(n_kv)
    asks = take(n_ask)
    new_angle = take(1)[0] if n_ask else None
    kv_out = take(1)[0]
    direct_out, passed_out = (None,) * 2 if kv_only else take(2)
    new_out = take(1)[0] if n_ask else None
    x, gain, tabs, normed, qkv, in_sem = take(6)
    attn = None if kv_only else take(1)[0]
    raw_s = take(1)[0] if n_ask else None
    rows = x.shape[0]
    heads = kv_out.shape[0] // 2
    shards = [idx[n_full + 2 * which + i] for i in range(2)]
    at = pl.ds(pl.multiple_of(shards[1] * rows, rows), rows)
    ready = load(
        [(gain_hbm, gain), (passed, x), (cos_hbm.at[at], tabs.at[0]), (sin_hbm.at[at], tabs.at[1])],
        in_sem,
    )
    ready[0].wait()
    if n_ask:
        here = idx[idx.shape[0] - 1].astype(f32)
        steps = asks[0].shape[0] // 2
        new = jnp.zeros((steps, x.shape[1]), f32)
        for ref in asks:
            wide = ref[...].astype(f32)
            new = jnp.where(wide[steps : steps + 1] == here, wide[:steps], new)
        fill = jnp.zeros((16 - steps, x.shape[1]), f32)
        normed[rows:] = norm_token_rows([new, fill], gain)
    ready[1].wait()
    norm_rows(x, normed, 0, gain)
    for copy in ready[2:]:
        copy.wait()
    for j in range(wq.shape[0]):
        acc = dot(normed[...], wq[j])
        qkv[j] = rotated_pair(acc[:rows], tabs.at[0], tabs.at[1], j)
        if n_ask:
            raw_s[j] = acc[rows : rows + raw_s.shape[1]]
    both = (direct, qkv)
    for i in range(2):
        for h in range(heads):
            kv_out[i * heads + h] = both[i][h * BLOCKS + BLOCKS - 1]
    if kv_only:
        return
    pieces = [(lambda h, ref=ref: ref[h * BLOCKS + BLOCKS - 1], idx[i]) for i, ref in enumerate(full)]
    others = [n for n in range(n_kv + 1) if n != which]
    for ref, n in zip(kvs, others):
        for i in range(2):
            pieces.append((lambda h, ref=ref, i=i: ref[i * heads + h], idx[n_full + 2 * n + i]))
    for i in range(2):
        pieces.append((lambda h, i=i: both[i][h * BLOCKS + BLOCKS - 1], shards[i]))
    for i in (1, 0):
        attend(lambda b, i=i: both[i][b], shards[i], pieces, plen[0, 0], attn, i * rows, heads)
    if n_ask:
        steps = new_angle.shape[0]
        raw = lambda b: raw_s[b, :steps]
        attend_new(raw, *spread(new_angle[...]), pieces, plen[0, 0], new_out, heads, steps)
    for j in range(wo.shape[0]):
        cols = slice(j * OUT_COLS, (j + 1) * OUT_COLS)
        part = dot(attn[...], wo[j]).astype(bf16)
        direct_out[:, cols] = part[:rows]
        passed_out[:, cols] = part[rows:]


def last_kernel(n_kv, n_ret, n_rows, low_rows, *refs):
    refs = list(refs)
    take = lambda n: [refs.pop(0) for _ in range(n)]
    idx, plen, slot, assign, own, sib = take(6)
    kvs = take(n_kv)
    decs = take(2)
    rets = take(n_ret)
    wo, own_part, sib_part, dec_part, attn = take(5)
    rows = own.shape[1]
    heads = kvs[0].shape[0] // 2
    pieces = [(lambda h, ref=ref: ref[h * BLOCKS + BLOCKS - 1], idx[i]) for i, ref in enumerate((own, sib))]
    for n, ref in enumerate(kvs):
        for i in range(2):
            pieces.append((lambda h, ref=ref, i=i: ref[i * heads + h], idx[2 + 2 * n + i]))
    for i, ref in enumerate((own, sib)):
        attend(lambda b, ref=ref: ref[b], idx[i], pieces, plen[0, 0], attn, i * rows, heads)
    pick = lax.rem(idx[idx.shape[0] - 1] - assign[0, 0] + n_ret, n_ret)
    new = rets[0][...].astype(f32)
    for k in range(1, n_ret):
        new = jnp.where(pick == k, rets[k][...].astype(f32), new)
    at = lax.rem(lax.broadcasted_iota(jnp.int32, new.shape, 0), n_rows)
    dec = jnp.where(at < low_rows, decs[0][...], decs[1][...])
    attn[2 * rows :] = jnp.where(at == slot[0, 0], new, dec).astype(bf16)
    for j in range(wo.shape[0]):
        part = dot(attn[...], wo[j]).astype(bf16)
        cols = slice(j * OUT_COLS, (j + 1) * OUT_COLS)
        own_part[:, cols] = part[:rows]
        sib_part[:, cols] = part[rows:]
        dec_part[:, cols] = part[2 * rows :]


def add_kernel(start, a, b, out):
    rows = out.shape[0]

    def step(i, _):
        at = pl.ds(pl.multiple_of(i * 16, 16), 16)
        to = pl.ds(pl.multiple_of(start + i * 16, 16), 16)
        out[at, :] = (a[at, :].astype(f32) + b[to, :].astype(f32)).astype(bf16)
        return 0

    lax.fori_loop(0, rows // 16, step, 0)


def base_kernel(shard_hbm, own, sib, out, shard, sem):
    copy = pltpu.make_async_copy(shard_hbm, shard, sem)
    copy.start()
    copy.wait()

    def step(i, _):
        at = pl.ds(pl.multiple_of(i * 16, 16), 16)
        out[at, :] = shard[at, :].astype(f32) + own[at, :].astype(f32) + sib[at, :].astype(f32)
        return 0

    lax.fori_loop(0, out.shape[0] // 16, step, 0)


def sum_kernel(count, base, *refs):
    parts, out, got, sems, out_sem = refs[:count], *refs[count:]
    pieces = sems.shape[1]
    rows = out.shape[0] // pieces
    at = [pl.ds(n * rows, rows) for n in range(pieces)]
    copies = [
        [pltpu.make_async_copy(part.at[at[n]], got.at[d, at[n]], sems.at[d, n]) for d, part in enumerate(parts)]
        for n in range(pieces)
    ]
    for copy in sum(copies, []):
        copy.start()
    done = []
    for n in range(pieces):
        here = slice(n * rows, (n + 1) * rows)
        total = base[here]
        for d in range(count):
            copies[n][d].wait()
            total = total + got[d, here].astype(f32)
        got[0, here] = total.astype(bf16)
        done.append(pltpu.make_async_copy(got.at[0, at[n]], out.at[at[n]], out_sem.at[n]))
        done[-1].start()
    for copy in done:
        copy.wait()


def dec_kernel(tokens, a, b, out):
    steps, n_rows = tokens.shape[:2]
    total = a[...].astype(f32) + b[...].astype(f32)
    for s in range(steps):
        rows = total[s * n_rows : (s + 1) * n_rows]
        out[s] = (tokens[s].astype(f32) + rows).astype(bf16)


def params(mib):
    return pltpu.CompilerParams(vmem_limit_bytes=mib << 20)


def layer(
    prompt, prompt_len, dec_tokens, cache_k, cache_v, cache_len, assign, slot, gain, w_qkv, w_out
):
    n_blk, n_pool, n_batch = lax.axis_size("blk"), lax.axis_size("pool"), lax.axis_size("batch")
    n_chip = n_blk // 2
    shard = prompt[0]
    rows, width = shard.shape
    steps, n_rows = dec_tokens.shape[:2]
    heads = w_qkv.shape[1] // (KINDS * HEAD_DIM)
    blocks = heads * BLOCKS
    attn_cols = heads * GROUP * HEAD_DIM
    out_blocks = width // OUT_COLS
    decs = steps * n_rows

    blk = lax.axis_index("blk")
    chip, core = lax.shift_right_logical(blk, 1), blk & 1
    batch = lax.axis_index("batch")
    at = jnp.arange(n_blk + 1, dtype=jnp.int32)
    far = lax.rem(chip + n_chip - lax.shift_right_logical(at, 1), n_chip)
    idx = jnp.where(at == n_blk, batch, 2 * far + ((core + at) & 1)).astype(jnp.int32)
    gain_row = gain.reshape(1, width)
    cos_t, sin_t = (jnp.asarray(t) for t in fixed_tables(n_blk * rows))
    ticks = jnp.arange(steps, dtype=jnp.int32)
    dec_angle = angle_tables(cache_len[:, None] + ticks[None, :])
    new_angle = angle_tables(prompt_len[0, 0] + ticks)

    swap = [(i, i ^ 1) for i in range(n_blk)]
    hop = lambda d: [(2 * c + k, 2 * ((c + d) % n_chip) + k) for c in range(n_chip) for k in range(2)]
    shift = [
        [
            (p * n_batch + b, ((p + n_pool // 2) % n_pool) * n_batch + (b + k) % n_batch)
            for p in range(n_pool)
            for b in range(n_batch)
        ]
        for k in range(n_batch)
    ]
    groups = ("pool", "batch")
    near = lambda x: pltpu.with_memory_space_constraint(x, pltpu.MemorySpace.VMEM)
    stay = lambda x: pltpu.with_memory_space_constraint(x, pltpu.MemorySpace.HBM)

    sib_x = lax.ppermute(shard, "blk", swap)
    far_x = []
    for d in range(1, n_chip):
        far_x.append(lax.ppermute(shard, "blk", hop(d)))

    own, sib, raw, wq, ask = pl.pallas_call(
        first_kernel,
        in_specs=[SMEM] * 3 + [HBM] * 7 + [ANY] * 2,
        out_specs=[VMEM] * 5,
        out_shape=[
            jax.ShapeDtypeStruct((blocks, rows, PAIR), bf16),
            jax.ShapeDtypeStruct((blocks, rows, PAIR), bf16),
            jax.ShapeDtypeStruct((n_rows, blocks, steps, PAIR), f32),
            pltpu.VMEM((blocks, width, PAIR), bf16),
            jax.ShapeDtypeStruct((2 * steps, width), bf16),
        ],
        scratch_shapes=[
            pltpu.VMEM((rows, width), bf16),
            pltpu.VMEM((rows, width), bf16),
            pltpu.VMEM((steps, n_rows, width), bf16),
            pltpu.VMEM((1, width), f32),
            pltpu.VMEM((4, rows, HEAD_DIM), f32),
            pltpu.VMEM((2 * rows + decs, width), bf16),
            pltpu.SemaphoreType.DMA((blocks,)),
            pltpu.SemaphoreType.DMA((8,)),
        ],
        compiler_params=params(10),
        name="first",
    )(
        idx, slot, assign, stay(shard), sib_x, stay(dec_tokens), stay(gain_row), stay(cos_t),
        stay(sin_t), stay(w_qkv), dec_angle, new_angle,
    )

    def project(which, x, loads):
        outs = [jax.ShapeDtypeStruct((blocks, rows, PAIR), bf16)]
        if loads:
            outs.append(pltpu.VMEM((out_blocks, attn_cols, OUT_COLS), bf16))
        return pl.pallas_call(
            functools.partial(project_kernel, which, loads),
            in_specs=[SMEM] + [HBM] * 4 + [VMEM] + [HBM] * loads,
            out_specs=[VMEM] * len(outs),
            out_shape=outs,
            scratch_shapes=[
                pltpu.VMEM((rows, width), bf16),
                pltpu.VMEM((1, width), f32),
                pltpu.VMEM((2, rows, HEAD_DIM), f32),
                pltpu.VMEM((rows, width), bf16),
                pltpu.SemaphoreType.DMA((4,)),
            ] + [pltpu.SemaphoreType.DMA((out_blocks,))] * loads,
            compiler_params=params(8),
            name="project",
        )(
            idx, x, stay(gain_row), stay(cos_t), stay(sin_t), near(wq),
            *([stay(w_out)] if loads else []),
        )

    asks = [lax.ppermute(ask, groups, perm) for perm in shift]

    cached = cache_k.shape[1]
    step_rows = min(2048, cached)
    count = cached // step_rows
    kv_width = heads * HEAD_DIM
    many = GROUP * steps * heads
    low_rows = max(n_rows // 4, 1)

    def decode(first, many_rows):
        return pl.pallas_call(
            functools.partial(decode_kernel, first),
            in_specs=[SMEM] * 2 + [VMEM] * 2 + [HBM] * 2,
            out_specs=VMEM,
            out_shape=jax.ShapeDtypeStruct((decs, attn_cols), f32),
            scratch_shapes=[
                pltpu.VMEM((many_rows, count, step_rows, kv_width), bf16),
                pltpu.VMEM((many_rows, count, step_rows, kv_width), bf16),
                pltpu.VMEM((many_rows, many, kv_width), bf16),
                pltpu.VMEM((many_rows, 16, kv_width), bf16),
                pltpu.VMEM((many_rows, 16, kv_width), bf16),
                pltpu.VMEM((many_rows, many, 1), f32),
                pltpu.VMEM((many_rows, many, 1), f32),
                pltpu.VMEM((many_rows, many, kv_width), f32),
                pltpu.SemaphoreType.DMA((many_rows, count)),
                pltpu.SemaphoreType.DMA((many_rows, count)),
            ],
            compiler_params=params(16),
            name="decode",
        )(cache_len, slot, raw, dec_angle, stay(cache_k), stay(cache_v))

    dec_low = decode(0, low_rows)
    dec_high = decode(low_rows, n_rows - low_rows)

    fronts, wo = [], None
    for n in range(n_chip - 1):
        passed = lax.ppermute(far_x[n], "blk", swap)
        outs = project(2 + 2 * n, far_x[n], n == 0)
        fronts.append((passed, outs[0]))
        if n == 0:
            wo = outs[1]

    def chunk(n, kvs, asks, kv_only):
        passed, direct = fronts[n]
        outs = [jax.ShapeDtypeStruct((2 * heads, rows, PAIR), bf16)]
        scratch = [
            pltpu.VMEM((rows, width), bf16),
            pltpu.VMEM((1, width), f32),
            pltpu.VMEM((2, rows, HEAD_DIM), f32),
            pltpu.VMEM((rows + (16 if asks else 0), width), bf16),
            pltpu.VMEM((blocks, rows, PAIR), bf16),
            pltpu.SemaphoreType.DMA((4,)),
        ]
        if not kv_only:
            outs += [jax.ShapeDtypeStruct((rows, width), bf16)] * 2
            scratch.append(pltpu.VMEM((2 * rows, attn_cols), bf16))
        extra = []
        if asks:
            outs.append(jax.ShapeDtypeStruct((decs, attn_cols), bf16))
            scratch.append(pltpu.VMEM((blocks, 8, PAIR), f32))
            extra = [*asks, new_angle]
        kernel = functools.partial(chunk_kernel, n, 2, len(kvs), len(asks), kv_only)
        return pl.pallas_call(
            kernel,
            in_specs=[SMEM] * 2 + [HBM] * 4 + [VMEM] * (5 + len(kvs) + len(extra)),
            out_specs=[VMEM] * len(outs),
            out_shape=outs,
            scratch_shapes=scratch,
            compiler_params=params(16),
            name="chunk",
        )(
            idx, prompt_len, passed, stay(gain_row), stay(cos_t), stay(sin_t),
            direct, near(wq), near(wo), own, sib, *kvs, *extra,
        )

    def add(a, b, start=0):
        return pl.pallas_call(
            functools.partial(add_kernel, start),
            in_specs=[VMEM] * 2,
            out_specs=VMEM,
            out_shape=jax.ShapeDtypeStruct(a.shape, bf16),
            compiler_params=params(8),
            name="add",
        )(a, b)

    kvs, back, fresh = [], [], None
    ahead = n_chip > 2
    if ahead:
        kvs = [chunk(n, [], [], True)[0] for n in range(n_chip - 1)]
    for n in range(n_chip - 1):
        final = n == n_chip - 2
        others = [kv for i, kv in enumerate(kvs) if i != n]
        outs = chunk(n, others, asks if final else [], False)
        if not ahead:
            kvs.append(outs[0])
        if final:
            fresh = outs[3]
        other = lax.ppermute(outs[2], "blk", swap)
        both = add(outs[1], other)
        back.append(lax.ppermute(both, "blk", hop(n_chip - 1 - n)))

    rets = []
    for perm in shift:
        rets.append(lax.ppermute(fresh, groups, perm))
    own_part, sib_part, dec_part = pl.pallas_call(
        functools.partial(last_kernel, len(kvs), n_batch, n_rows, low_rows),
        in_specs=[SMEM] * 4 + [VMEM] * (5 + len(kvs) + n_batch),
        out_specs=[VMEM] * 3,
        out_shape=[
            jax.ShapeDtypeStruct((rows, width), bf16),
            jax.ShapeDtypeStruct((rows + decs, width), bf16),
            jax.ShapeDtypeStruct((decs, width), bf16),
        ],
        scratch_shapes=[
            pltpu.VMEM((2 * rows + decs, attn_cols), bf16),
        ],
        compiler_params=params(12),
        name="last",
    )(idx, prompt_len, slot, assign, own, sib, *kvs, dec_low, dec_high, *rets, near(wo))
    from_sib = lax.ppermute(sib_part, "blk", swap)

    total = add(dec_part, from_sib, rows)
    reach = 1
    while reach < n_chip:
        other = lax.ppermute(total, "blk", [(i, i ^ (2 * reach)) for i in range(n_blk)])
        reach *= 2
        if reach < n_chip:
            total = add(total, other)
    dec_out = pl.pallas_call(
        dec_kernel,
        in_specs=[VMEM] * 3,
        out_specs=VMEM,
        out_shape=jax.ShapeDtypeStruct(dec_tokens.shape, bf16),
        compiler_params=params(8),
        name="dec",
    )(dec_tokens, total, other)
    base = pl.pallas_call(
        base_kernel,
        in_specs=[HBM, VMEM, VMEM],
        out_specs=VMEM,
        out_shape=jax.ShapeDtypeStruct((rows, width), f32),
        scratch_shapes=[pltpu.VMEM((rows, width), bf16), pltpu.SemaphoreType.DMA],
        compiler_params=params(8),
        name="base",
    )(stay(shard), own_part, from_sib)
    pieces = 4
    result = pl.pallas_call(
        functools.partial(sum_kernel, n_chip - 1),
        in_specs=[VMEM] + [HBM] * (n_chip - 1),
        out_specs=HBM,
        out_shape=jax.ShapeDtypeStruct((rows, width), bf16),
        scratch_shapes=[
            pltpu.VMEM((n_chip - 1, rows, width), bf16),
            pltpu.SemaphoreType.DMA((n_chip - 1, pieces)),
            pltpu.SemaphoreType.DMA((pieces,)),
        ],
        compiler_params=params(10),
        name="sum",
    )(base, *back)
    return (result[None], dec_out)


def solution(mesh):
    return jax.shard_map(
        layer,
        mesh=mesh,
        in_specs=(
            P(("pool", "batch"), "blk", None),
            P("pool", "batch"),
            P(None, ("pool", "batch"), None),
            P(("pool", "batch"), None, "blk"),
            P(("pool", "batch"), None, "blk"),
            P(("pool", "batch")),
            P("pool", "batch"),
            P("pool", "batch"),
            P(),
            P(None, "blk"),
            P("blk", None),
        ),
        out_specs=(P(("pool", "batch"), "blk", None), P(None, ("pool", "batch"), None)),
        check_vma=False,
    )
```
